128 devices in a mesh: px: 8 (over y_lo, x), py: 16 (over z, y_hi, core).
Axes of the slice: x: 4, y: 4 (y_hi: 2, y_lo: 2; y = y_hi * 2 + y_lo), z: 4, core: 2. Of those that a mesh axis runs over, the one named last changes fastest.
Arguments:
- photons: float32 [4096, 128], P(('px', 'py')), may hold values from 50 to 1000
- halo_cells: int32 [4096, 128], P(('px', 'py')), may hold values from 0 to 442367
- halo_counts: int32 [4096], P(('px', 'py')), may hold values from 1 to 128
- owners: int32 [4096, 1], P(('px', 'py')), may hold values from 0 to 15; in each aligned block of 32 rows (0 to 31, 32 to 63, ...) at most 4 rows name the same one
- density: float32 [384, 384, 384], P('px', 'py'), may hold values from 0.02 to 50
Outputs:
- fraction: float32 [384, 384, 384], P('px', 'py')
The draws below stay inside these ranges and needn't reach their ends.
Inputs may be any that keep to these rules, and one draw needn't show every extreme that they name: The halos of a block all lie in pencil owners[b] of the block's own slab. Among the 32 blocks of one device no owner appears more than 4 times, a bound that some block reaches. Slots at or past halo_counts[b] are not live and carry arbitrary values. `halo_cells`: A cell index within the owner pencil is (x * 24 + y) * 384 + z with x, y, z local to that pencil.
All inputs are finite; a program needn't handle non-finite values.
Results may differ from the reference program's by a relative error of at most 0.0003.
Values sent between devices are 32-bit elements; how exact they have to be, the bound alone decides.
A program may use at most 128 MiB of HBM per device.

```python
import math
import jax
import jax.numpy as jnp
import numpy as np
from jax import lax

NG = 384
SLOTS = 128
CAP = 4
RADIUS = 20
BLK_DEV = 32
CX = 48
CY = 24
HROWS = 4096
N_PY = 16


def draw_density(key, part):
    subkeys = jax.random.split(jax.random.fold_in(key, 7), 4)
    wave_numbers = jax.random.randint(subkeys[0], (4, 3), 1, 4)
    flip_signs = jax.random.randint(subkeys[1], (4, 3), 0, 2) * 2 - 1
    wave_numbers = wave_numbers * flip_signs
    phases = jax.random.uniform(subkeys[2], (4,), jnp.float32, -jnp.pi, jnp.pi)
    coords = jnp.arange(NG, dtype=jnp.int32)
    smooth = jnp.zeros((NG, NG, NG), jnp.float32)
    for number in range(4):
        along_x = wave_numbers[number, 0] * coords % NG
        along_y = wave_numbers[number, 1] * coords % NG
        along_z = wave_numbers[number, 2] * coords % NG
        total = (along_x[:, None, None] + along_y[None, :, None] + along_z[None, None, :]) % NG
        smooth = smooth + jnp.cos(total.astype(jnp.float32) * (2.0 * jnp.pi / NG) + phases[number])
    smooth = smooth / jnp.sqrt(2.0)
    rough_part = jnp.clip(1.8 * jax.random.normal(subkeys[3], (NG, NG, NG), jnp.float32), -4.0, 4.0) - 1.4
    amplitude = 0.8
    return jnp.clip(jnp.exp(amplitude * smooth + rough_part), 0.02, 50.0).astype(jnp.float32)


def place_ends(result, own_key, smallest, top_value):
    spot = [jax.random.randint(jax.random.fold_in(own_key, axis), (), 0, length) for axis, length in enumerate(result.shape)]
    main_axis = result.shape.index(max(result.shape))
    neighbour = spot[:main_axis] + [(spot[main_axis] + 1) % result.shape[main_axis]] + spot[main_axis + 1:]
    return result.at[tuple(spot)].set(smallest).at[tuple(neighbour)].set(top_value)


def level_of(key, extent, pieces, low, largest):
    factor_of = 1.0
    for axis_at, shards_of in pieces:
        heights = jax.random.uniform(jax.random.fold_in(jax.random.fold_in(key, 6), axis_at), (shards_of,), jnp.float32, low / len(pieces), largest / len(pieces))
        factor_of = factor_of * jnp.repeat(jnp.exp(heights), extent[axis_at] // shards_of).reshape((-1,) + (1,) * (len(extent) - 1 - axis_at))
    return factor_of


def deal_out(stream_key, own, number, rows, amount, top, most, skew):
    sequence = jax.random.permutation(stream_key, amount)
    crowded, usual = shares(amount, rows * top, most, skew, True), shares(amount, rows * top, most, skew, False)
    places = jnp.arange(amount)

    def named(sizes, rotation):
        used = int((sizes > 0).sum())
        fixed = max(1, used // 4)
        passed = fixed + (places - fixed + rotation * (used - fixed)) % max(1, amount - fixed)
        return jnp.zeros((amount,), jnp.int32).at[sequence[jnp.where(places < fixed, places, passed)]].set(jnp.asarray(sizes, jnp.int32))

    sizes = jnp.where(number % 4 == 0, named(crowded, number // 4), named(usual, number - number // 4 - 1))
    mixed = jax.random.permutation(jax.random.fold_in(own, 3), amount)
    giver, receiver = mixed[0:amount // 2 * 2:2], mixed[1:amount // 2 * 2:2]
    margin = jnp.minimum(sizes[giver] - 1, most - sizes[receiver]) // 2
    margin = jnp.where((giver == sequence[0]) | (receiver == sequence[0]) | (sizes[receiver] == 0), 0, jnp.maximum(margin, 0))
    passed = jax.random.randint(jax.random.fold_in(own, 4), (amount // 2,), 0, 1 << 20) % (margin + 1)
    sizes = sizes.at[giver].add(-passed).at[receiver].add(passed)
    items = jnp.searchsorted(jnp.cumsum(sizes), jnp.arange(rows * top), side="right").astype(jnp.int32)
    table = items.reshape(top, rows).T
    table = table[jax.random.permutation(jax.random.fold_in(own, 1), rows)]
    rotation = jax.random.randint(jax.random.fold_in(own, 2), (rows, 1), 0, top)
    return jnp.take_along_axis(table, (jnp.arange(top)[None, :] + rotation) % top, axis=1)


def shares(count, total, reach, slope, full):
    weights = [(1 << 20) // math.isqrt(rank ** slope) + 1 for rank in range(1, count + 1)]
    largest = reach if full else min(reach, max(-(-total // count), total * weights[0] // sum(weights)))
    least = 1 if total - largest >= count - 1 else 0
    counts, spare = [largest] + [least] * (count - 1), total - largest - least * (count - 1)
    while spare > 0:
        free = [i for i in range(1, count) if counts[i] < largest] or [i for i in range(1, count) if counts[i] < reach]
        whole, budget = sum([weights[i] for i in free]), spare
        for i in free:
            extra = min(reach - counts[i], max(1, budget * weights[i] // whole), spare)
            counts[i] = counts[i] + extra
            spare = spare - extra
    return np.array(counts)


def setup_inputs(seed: int = 0) -> dict:
    seeds = jax.random.split(jax.random.key(seed), 6)
    photons = jnp.clip(jnp.exp(math.log(1000.0) - 2.9957323 * jax.random.uniform(seeds[0], (HROWS, SLOTS), jnp.float32) ** level_of(seeds[0], (HROWS, SLOTS), ((0, 128),), -0.2, 0.2)), 50.0, 1000.0)
    halo_cells = place_ends(jax.random.randint(seeds[1], (HROWS, SLOTS), 0, CX * CY * NG), jax.random.fold_in(seeds[1], 1), 0, (CX * CY * NG) - 1).astype(jnp.int32)
    halo_counts = place_ends(jax.random.randint(seeds[2], (HROWS,), 1, SLOTS + 1), jax.random.fold_in(seeds[2], 1), 1, SLOTS).astype(jnp.int32)
    owners_keys = jax.random.split(jax.random.fold_in(seeds[3], 1), HROWS // BLK_DEV)
    owners_turns = jax.random.permutation(jax.random.fold_in(seeds[3], 3), HROWS // BLK_DEV)
    owners = jax.vmap(lambda own, number: deal_out(jax.random.fold_in(seeds[3], 2), own, number, BLK_DEV, N_PY, 1, CAP, 2))(owners_keys, owners_turns).reshape((HROWS, 1))
    density = draw_density(jax.random.fold_in(seeds[5], 71), 0)
    return dict(photons=photons, halo_cells=halo_cells, halo_counts=halo_counts, owners=owners, density=density)


def top_hat(freq_x, freq_y, freq_z):
    radial = jnp.sqrt(freq_x * freq_x + freq_y * freq_y + freq_z * freq_z) * (2.0 * jnp.pi * RADIUS / NG)
    safe = jnp.where(radial > 0, radial, 1.0)
    value = 3.0 * (jnp.sin(safe) - safe * jnp.cos(safe)) / (safe * safe * safe)
    return jnp.where(radial > 0, value, 1.0)

def reference(photons, halo_cells, halo_counts, owners, density):
    row_count = photons.shape[0]
    row_index = jnp.arange(row_count, dtype=jnp.int32)
    slab_index = row_index // (N_PY * BLK_DEV)
    local_x = halo_cells // (CY * NG)
    local_y = halo_cells // NG % CY
    local_z = halo_cells % NG
    global_x = slab_index[:, None] * CX + local_x
    global_y = owners[:, 0:1] * CY + local_y
    flat_index = ((global_x * NG + global_y) * NG + local_z).astype(jnp.int32)
    live_slots = jnp.arange(photons.shape[1], dtype=jnp.int32)[None, :] < halo_counts[:, None]
    weights = jnp.where(live_slots, photons, jnp.zeros_like(photons))
    field = jnp.zeros((NG * NG * NG,), photons.dtype).at[flat_index.reshape(-1)].add(weights.reshape(-1))
    field = field.reshape(NG, NG, NG)
    packed = lax.complex(field, density)
    spectrum = jnp.fft.fftn(packed)
    index_values = jnp.arange(NG, dtype=jnp.int32)
    signed_frequency = jnp.where(index_values < NG // 2, index_values, index_values - NG).astype(density.dtype)
    window = top_hat(signed_frequency[:, None, None], signed_frequency[None, :, None], signed_frequency[None, None, :])
    smoothed = jnp.fft.ifftn(spectrum * window)
    photon_smooth = jnp.real(smoothed)
    density_smooth = jnp.imag(smoothed)
    fraction = jnp.clip(photon_smooth / jnp.maximum(density_smooth, 0.5), 0.0, 1.0)
    return fraction.astype(jnp.float32)
```

```python
import functools

import jax
import jax.numpy as jnp
import numpy as np
from jax import lax
from jax.experimental import pallas as pl
from jax.experimental.pallas import tpu as pltpu
from jax.sharding import PartitionSpec as P

NG = 384
SLOTS = 128
CAP = 4
RADIUS = 20
DEV = 128
CELLS = 1152
PLANE = 2 * CELLS
HEAD = 72
TAIL = 56
LIMIT = 60 * 1024 * 1024
F32 = jnp.float32
BF16 = jnp.bfloat16
VMEM = pltpu.VMEM
SMEM = pltpu.SMEM


def cut(v):
    hi = v.astype(BF16)
    return hi, (v - hi.astype(F32)).astype(BF16)


def cut_np(v):
    v = np.asarray(v, np.float32)
    hi = v.astype(jnp.bfloat16)
    lo = (v - hi.astype(np.float32)).astype(jnp.bfloat16)
    return hi, lo


NN = (((1,), (0,)), ((), ()))
NT = (((1,), (1,)), ((), ()))


def mm(a, b, dims):
    return lax.dot_general(a, b, dims, preferred_element_type=F32)


def mm3(ah, al, bh, bl, dims=NN):
    return mm(ah, bh, dims) + (mm(ah, bl, dims) + mm(al, bh, dims))


def kz_first():
    return np.arange(1, DEV + 1)


def kz_second():
    k = np.zeros(DEV, np.int64)
    k[:63] = 129 + np.arange(63)
    k[63] = 0
    k[64] = NG // 2
    k[65:] = 129 + np.arange(63)
    return k


def z_tables():
    z = np.arange(NG)

    def c(k):
        return np.cos(2 * np.pi * ((k[:, None] * z[None]) % NG) / NG)

    def s(k):
        return np.sin(2 * np.pi * ((k[:, None] * z[None]) % NG) / NG)

    first = np.concatenate([c(kz_first()), s(kz_first())])
    k = kz_second()
    d = np.arange(DEV)[:, None]
    special = (d == 63) | (d == 64)
    g_re = np.where(d < 63, c(k), 0.0)
    g_im = np.where(d < 63, s(k), 0.0) + np.where(special, c(k), 0.0)
    f_re = np.where(d > 62, c(k), 0.0)
    f_im = np.where(d > 64, s(k), 0.0)
    second_g = np.concatenate([g_re[:HEAD], g_im[:HEAD]])
    second_f = np.concatenate([f_re[TAIL:], f_im[TAIL:]])
    return first, second_g, second_f


def mix(left, right):
    i = np.arange(left * right)
    a, b = i // right, i % right
    ph = -2j * np.pi * (np.outer(a, a) / left + np.outer(b, b) / right)
    return np.exp(ph)


def row_matrix(sign):
    m = mix(8, 16)
    re, im = m.real, sign * m.imag
    return np.block([[re, -im], [im, re]])


def lane_matrix(sign):
    m = mix(16, 8)
    re, im = m.real, sign * m.imag
    return np.block([[re, im], [-im, re]])


def freq_parts():
    row = lax.broadcasted_iota(jnp.int32, (CELLS, 128), 0)
    lane = lax.broadcasted_iota(jnp.int32, (CELLS, 128), 1)
    m, s = row // 128, row % 128
    return s // 16, s % 16, m // 3, m % 3, lane // 8, lane % 8


def twiddles():
    ax, ay, bx, by, cx, cy = freq_parts()
    w = 2.0 * jnp.pi / NG
    one = ((ax * bx * 16 + ay * by * 8) % NG).astype(F32) * w
    two = ((cx * (ax + 8 * bx) + cy * (ay + 16 * by)) % NG).astype(F32) * w
    return jnp.cos(one), -jnp.sin(one), jnp.cos(two), -jnp.sin(two)


def signed(k):
    return jnp.where(k < NG // 2, k, k - NG).astype(F32)


def top_hat(freq_x, freq_y, freq_z):
    radial = jnp.sqrt(freq_x * freq_x + freq_y * freq_y + freq_z * freq_z) * (2.0 * jnp.pi * RADIUS / NG)
    safe = jnp.where(radial > 0, radial, 1.0)
    value = 3.0 * (jnp.sin(safe) - safe * jnp.cos(safe)) / (safe * safe * safe)
    return jnp.where(radial > 0, value, 1.0)


def window(me, kz):
    ax, ay, bx, by, cx, cy = freq_parts()
    kx, ky = ax + 8 * bx + 24 * cx, ay + 16 * by + 48 * cy
    k = jnp.asarray(kz, jnp.int32)[me]
    scale = jnp.where((k == 0) | (k == NG // 2), 1.0, 2.0) / float(NG) ** 3
    return top_hat(signed(kx), signed(ky), signed(k)) * scale


def call(body, out_shape, args, scratch, spaces=None, flops=0, nbytes=0, name=None, **params):
    spaces = spaces or [VMEM] * len(args)
    outs = jax.tree.map(lambda _: pl.BlockSpec(memory_space=VMEM), out_shape)
    return pl.pallas_call(
        body,
        out_shape=out_shape,
        in_specs=[pl.BlockSpec(memory_space=s) for s in spaces],
        out_specs=outs,
        scratch_shapes=scratch,
        compiler_params=pltpu.CompilerParams(vmem_limit_bytes=LIMIT, **params),
        cost_estimate=pl.CostEstimate(flops=flops, bytes_accessed=nbytes, transcendentals=0),
        name=name,
    )(*args)


def prep_body(ph_ref, cell_ref, count_ref, own_col, own_row, out_ref):
    lane = lax.broadcasted_iota(jnp.int32, (32, SLOTS), 1)
    live = lane < count_ref[...]
    w = jnp.where(live, ph_ref[...], 0.0)
    cells = jnp.where(live, cell_ref[...], 0).astype(F32)
    before = lax.broadcasted_iota(jnp.int32, (32, 32), 0) < lax.broadcasted_iota(jnp.int32, (32, 32), 1)
    same = (own_col[...] == own_row[...]) & before
    rank = jnp.sum(jnp.where(same, 1.0, 0.0), axis=0, keepdims=True).astype(jnp.int32)
    place = own_row[...] * (2 * CAP) + rank
    rows = lax.broadcasted_iota(jnp.int32, (DEV, 32), 0)
    total = jnp.zeros((DEV, SLOTS), F32)
    for values, shift in ((w, 0), (cells, CAP)):
        hot = jnp.where(rows == place + shift, 1.0, 0.0).astype(BF16)
        hi = values.astype(BF16)
        rest = values - hi.astype(F32)
        mid = rest.astype(BF16)
        low = (rest - mid.astype(F32)).astype(BF16)
        total = total + ((mm(hot, hi, NN) + mm(hot, mid, NN)) + mm(hot, low, NN))
    out_ref[...] = total.reshape(16, 2 * CAP, SLOTS)


def density_body(dens, t0h, t0l, t1h, t1l, x0, y1, gh, gl):
    for m in range(9):
        xh, lh = m // 3, m % 3
        rows = [dens[(16 * xh + xl) * 24 + 8 * lh : (16 * xh + xl) * 24 + 8 * lh + 8, :] for xl in range(16)]
        hi, lo = cut(jnp.concatenate(rows, axis=0))
        gh[m * 128 : (m + 1) * 128, :] = hi
        gl[m * 128 : (m + 1) * 128, :] = lo
    res = mm3(t0h[...], t0l[...], gh[...], gl[...], NT)
    x0[:, 0, :CELLS] = res[:DEV]
    x0[:, 0, CELLS:] = res[DEV:]
    y1[...] = mm3(t1h[...], t1l[...], gh[...], gl[...], NT)


BUFS = 4
UNROLL = 8


def paint_body(cnt, idx, ph, t0h, t0l, t1h, t1l, y1, x12, b0, b1, b2, b3, fh, fl):
    bufs = (b0, b1, b2, b3)
    zero = jnp.zeros((128, 128), F32)

    def clear(i, carry):
        at = pl.multiple_of(i * 128, 128)
        for b in bufs:
            b[pl.ds(at, 128), :] = zero
        return carry

    lax.fori_loop(0, 27, clear, 0)
    lane = lax.broadcasted_iota(jnp.int32, (1, 128), 1)

    def one_row(r, carry):
        def step(jb, inner):
            for u in range(UNROLL):
                j = jb * UNROLL + u
                at = idx[r, j]
                b = bufs[u % BUFS]
                row = lax.shift_right_logical(at, 7)
                here = lane == lax.bitwise_and(at, 127)
                b[pl.ds(row, 1), :] = b[pl.ds(row, 1), :] + jnp.where(here, ph[r, j], 0.0)
            return inner

        return lax.fori_loop(0, (cnt[r] + UNROLL - 1) // UNROLL, step, carry)

    lax.fori_loop(0, 16 * CAP, one_row, 0)
    for m in range(9):
        for zc in range(3):
            at = (zc * 9 + m) * 128
            v = (b0[at : at + 128, :] + b1[at : at + 128, :]) + (b2[at : at + 128, :] + b3[at : at + 128, :])
            hi, lo = cut(v)
            fh[m * 128 : (m + 1) * 128, zc * 128 : (zc + 1) * 128] = hi
            fl[m * 128 : (m + 1) * 128, zc * 128 : (zc + 1) * 128] = lo
    part = mm3(t1h[...], t1l[...], fh[...], fl[...], NT)
    for c in range(2):
        x12[:TAIL, 0, c * CELLS : (c + 1) * CELLS] = y1[c * HEAD : c * HEAD + TAIL, :]
        x12[TAIL:HEAD, 0, c * CELLS : (c + 1) * CELLS] = (
            y1[c * HEAD + TAIL : (c + 1) * HEAD, :] + part[c * HEAD : c * HEAD + HEAD - TAIL]
        )
        x12[HEAD:, 0, c * CELLS : (c + 1) * CELLS] = part[c * HEAD + HEAD - TAIL : (c + 1) * HEAD]
    res = mm3(t0h[...], t0l[...], fh[...], fl[...], NT)
    x12[:, 0, PLANE : PLANE + CELLS] = res[:DEV]
    x12[:, 0, PLANE + CELLS :] = res[DEV:]


ROOT = 0.8660254037844386


def three(a, b, c, inverse):
    tr, ti = b[0] + c[0], b[1] + c[1]
    dr, di = ROOT * (b[0] - c[0]), ROOT * (b[1] - c[1])
    er, ei = a[0] - 0.5 * tr, a[1] - 0.5 * ti
    one, two = (er + di, ei - dr), (er - di, ei + dr)
    return (a[0] + tr, a[1] + ti), *((two, one) if inverse else (one, two))


def nine(v, inverse):
    v = list(v)
    for x in range(3):
        v[3 * x : 3 * x + 3] = three(*v[3 * x : 3 * x + 3], inverse)
    for y in range(3):
        v[y], v[y + 3], v[y + 6] = three(v[y], v[y + 3], v[y + 6], inverse)
    return v


def turn(v, c, s):
    return v[0] * c - v[1] * s, v[0] * s + v[1] * c


RB = 16


def planes_body(n, x, w, ah, al, bh, bl, ch, cl, dh, dl, c1, s1, c2, s2, y, wide, tall, uh, ul, vh, vl):
    for p in range(n):
        base = p * PLANE
        for c in range(2):
            wide[c * DEV : (c + 1) * DEV, :] = x[:, 0, base + c * CELLS : base + (c + 1) * CELLS]
        hi, lo = cut(wide[...])
        wide[...] = mm3(ah[...], al[...], hi, lo)

        def forward(i, carry):
            r = pl.multiple_of(i * RB, RB)
            v = []
            for m in range(9):
                cols = slice(m * 128, (m + 1) * 128)
                t = pl.ds(m * 128 + r, RB)
                u = (wide[pl.ds(r, RB), cols], wide[pl.ds(DEV + r, RB), cols])
                v.append(turn(u, c1[t, :], s1[t, :]))
            for m, u in enumerate(nine(v, False)):
                t = pl.ds(m * 128 + r, RB)
                for c, part in enumerate(turn(u, c2[t, :], s2[t, :])):
                    hi, lo = cut(part)
                    uh[t, c * 128 : (c + 1) * 128] = hi
                    ul[t, c * 128 : (c + 1) * 128] = lo
            return carry

        lax.fori_loop(0, DEV // RB, forward, 0)
        mid = mm3(uh[...], ul[...], ch[...], cl[...])
        win = w[p]
        for c in range(2):
            hi, lo = cut(mid[:, c * 128 : (c + 1) * 128] * win)
            uh[:, c * 128 : (c + 1) * 128] = hi
            ul[:, c * 128 : (c + 1) * 128] = lo
        tall[...] = mm3(uh[...], ul[...], dh[...], dl[...])

        def backward(i, carry):
            r = pl.multiple_of(i * RB, RB)
            v = []
            for m in range(9):
                t = pl.ds(m * 128 + r, RB)
                v.append(turn((tall[t, :128], tall[t, 128:]), c2[t, :], -s2[t, :]))
            for m, u in enumerate(nine(v, True)):
                t = pl.ds(m * 128 + r, RB)
                cols = slice(m * 128, (m + 1) * 128)
                for c, part in enumerate(turn(u, c1[t, :], -s1[t, :])):
                    hi, lo = cut(part)
                    vh[pl.ds(c * DEV + r, RB), cols] = hi
                    vl[pl.ds(c * DEV + r, RB), cols] = lo
            return carry

        lax.fori_loop(0, DEV // RB, backward, 0)
        back = mm3(bh[...], bl[...], vh[...], vl[...])
        for c in range(2):
            y[:, 0, base + c * CELLS : base + (c + 1) * CELLS] = back[c * DEV : (c + 1) * DEV]


def last_body(r0, r12, gth, gtl, fth, ftl, out, stack, ga, fa):
    for c in range(2):
        stack[c * DEV : (c + 1) * DEV, :] = r0[:, 0, c * CELLS : (c + 1) * CELLS]
        stack[2 * DEV + c * HEAD : 2 * DEV + (c + 1) * HEAD, :] = r12[:HEAD, 0, c * CELLS : (c + 1) * CELLS]
    hi, lo = cut(stack[...])
    ga[...] = mm3(gth[...], gtl[...], hi, lo)
    for c in range(2):
        stack[c * DEV : (c + 1) * DEV, :] = r12[:, 0, PLANE + c * CELLS : PLANE + (c + 1) * CELLS]
        stack[2 * DEV + c * HEAD : 2 * DEV + (c + 1) * HEAD, :] = r12[TAIL:, 0, c * CELLS : (c + 1) * CELLS]
    hi, lo = cut(stack[...])
    fa[...] = mm3(fth[...], ftl[...], hi, lo)
    for m in range(9):
        xh, lh = m // 3, m % 3
        cols = slice(m * 128, (m + 1) * 128)
        frac = jnp.clip(fa[:, cols] / jnp.maximum(ga[:, cols], 0.5), 0.0, 1.0)
        turned = frac.T
        for xl in range(16):
            at = (16 * xh + xl) * 24 + 8 * lh
            out[at : at + 8, :] = turned[xl * 8 : xl * 8 + 8, :]


def sds(*shape, dtype=F32):
    return jax.ShapeDtypeStruct(shape, dtype)


def exchange(a):
    return lax.all_to_all(a, ("px", "py"), split_axis=0, concat_axis=0, tiled=True)


def planes(x, w, tabs):
    n = w.shape[0]
    return call(
        functools.partial(planes_body, n),
        sds(DEV, 1, n * PLANE),
        (x, w, *tabs),
        [VMEM((256, CELLS), F32), VMEM((CELLS, 256), F32)]
        + [VMEM((CELLS, 256), BF16)] * 2
        + [VMEM((256, CELLS), BF16)] * 2,
        flops=n * 4 * 3 * 2 * 256 * 256 * CELLS,
        nbytes=n * PLANE * DEV * 8,
        name="planes",
    )


def on_device(photons, halo_cells, halo_counts, owners, density):
    first, second_g, second_f = z_tables()
    t0 = [jnp.asarray(t) for t in cut_np(first)]
    t1g = [jnp.asarray(t) for t in cut_np(second_g)]
    t1f = [jnp.asarray(t) for t in cut_np(second_f)]
    back_g = [jnp.asarray(t) for t in cut_np(np.concatenate([first, second_g]).T)]
    back_f = [jnp.asarray(t) for t in cut_np(np.concatenate([first, second_f]).T)]
    mats = []
    for m in (row_matrix(1), row_matrix(-1), lane_matrix(1), lane_matrix(-1)):
        mats += [jnp.asarray(t) for t in cut_np(m)]
    me = lax.axis_index(("px", "py"))

    send = call(
        prep_body,
        sds(16, 2 * CAP, SLOTS),
        (photons, halo_cells, halo_counts.reshape(32, 1), owners, owners.reshape(1, 32)),
        [],
        flops=1 << 20,
        nbytes=1 << 17,
        name="prep",
    )
    got = lax.all_to_all(send, "py", split_axis=0, concat_axis=0, tiled=True)
    x0, y1 = call(
        density_body,
        (sds(DEV, 1, PLANE), sds(2 * HEAD, CELLS)),
        (density.reshape(CELLS, NG), *t0, *t1g),
        [VMEM((CELLS, NG), BF16)] * 2,
        flops=6 * 400 * NG * CELLS,
        nbytes=4 << 20,
        name="density",
    )
    x0 = exchange(x0)
    ph = got[:, :CAP].reshape(16 * CAP, SLOTS)
    cell = got[:, CAP:].reshape(16 * CAP, SLOTS).astype(jnp.int32)
    cnt = jnp.sum((ph > 0).astype(jnp.int32), axis=1)
    gx, gy, gz = cell // (24 * NG), cell // NG % 24, cell % NG
    chunk = gx // 16 * 3 + gy // 8
    idx = (((gz // 128) * 9 + chunk) * 128 + gx % 16 * 8 + gy % 8) * 128 + gz % 128
    x12 = call(
        paint_body,
        sds(DEV, 1, 2 * PLANE),
        (cnt, idx, ph, *t0, *t1f, y1),
        [VMEM((3 * CELLS, 128), F32)] * BUFS + [VMEM((CELLS, NG), BF16)] * 2,
        spaces=[SMEM] * 3 + [VMEM] * 5,
        flops=6 * 400 * NG * CELLS * 3,
        nbytes=4 << 20,
        name="paint",
    )
    x12 = exchange(x12)
    tabs = (*mats, *twiddles())
    r0 = planes(x0, window(me, kz_first())[None], tabs)
    r0 = exchange(r0)
    w12 = jnp.stack([window(me, kz_second()), window(me, kz_first())])
    r12 = exchange(planes(x12, w12, tabs))
    out = call(
        last_body,
        sds(CELLS, NG),
        (r0, r12, *back_g, *back_f),
        [VMEM((400, CELLS), F32), VMEM((NG, CELLS), F32), VMEM((NG, CELLS), F32)],
        flops=6 * 2 * 400 * NG * CELLS,
        nbytes=6 << 20,
        name="last",
    )
    return out.reshape(48, 24, NG)


def solution(mesh):
    placed = (
        P(("px", "py"), None),
        P(("px", "py"), None),
        P(("px", "py")),
        P(("px", "py"), None),
        P("px", "py", None),
    )
    return jax.shard_map(
        on_device, mesh=mesh, in_specs=placed, out_specs=P("px", "py", None), check_vma=False
    )
```

```python
import functools

import jax
import jax.numpy as jnp
import numpy as np
from jax import lax
from jax.experimental import pallas as pl
from jax.experimental.pallas import tpu as pltpu
from jax.sharding import PartitionSpec as P

NG = 384
SLOTS = 128
CAP = 4
RADIUS = 20
DEV = 128
CELLS = 1152
PLANE = 2 * CELLS
HEAD = 72
TAIL = 56
LIMIT = 60 * 1024 * 1024
F32 = jnp.float32
BF16 = jnp.bfloat16
VMEM = pltpu.VMEM
SMEM = pltpu.SMEM


def cut(v):
    hi = v.astype(BF16)
    return hi, (v - hi.astype(F32)).astype(BF16)


def cut_np(v):
    v = np.asarray(v, np.float32)
    hi = v.astype(jnp.bfloat16)
    lo = (v - hi.astype(np.float32)).astype(jnp.bfloat16)
    return hi, lo


NN = (((1,), (0,)), ((), ()))
NT = (((1,), (1,)), ((), ()))


def mm(a, b, dims):
    return lax.dot_general(a, b, dims, preferred_element_type=F32)


def mm3(ah, al, bh, bl, dims=NN):
    return mm(ah, bh, dims) + (mm(ah, bl, dims) + mm(al, bh, dims))


def kz_first():
    return np.arange(1, DEV + 1)


def kz_second():
    k = np.zeros(DEV, np.int64)
    k[:63] = 129 + np.arange(63)
    k[63] = 0
    k[64] = NG // 2
    k[65:] = 129 + np.arange(63)
    return k


def z_tables():
    z = np.arange(NG)

    def c(k):
        return np.cos(2 * np.pi * ((k[:, None] * z[None]) % NG) / NG)

    def s(k):
        return np.sin(2 * np.pi * ((k[:, None] * z[None]) % NG) / NG)

    first = np.concatenate([c(kz_first()), s(kz_first())])
    k = kz_second()
    d = np.arange(DEV)[:, None]
    special = (d == 63) | (d == 64)
    g_re = np.where(d < 63, c(k), 0.0)
    g_im = np.where(d < 63, s(k), 0.0) + np.where(special, c(k), 0.0)
    f_re = np.where(d > 62, c(k), 0.0)
    f_im = np.where(d > 64, s(k), 0.0)
    second_g = np.concatenate([g_re[:HEAD], g_im[:HEAD]])
    second_f = np.concatenate([f_re[TAIL:], f_im[TAIL:]])
    return first, second_g, second_f


def mix(left, right):
    i = np.arange(left * right)
    a, b = i // right, i % right
    ph = -2j * np.pi * (np.outer(a, a) / left + np.outer(b, b) / right)
    return np.exp(ph)


def row_matrix(sign):
    m = mix(8, 16)
    re, im = m.real, sign * m.imag
    return np.block([[re, -im], [im, re]])


def lane_matrix(sign):
    m = mix(16, 8)
    re, im = m.real, sign * m.imag
    return np.block([[re, im], [-im, re]])


def twiddles():
    row, lane = np.arange(CELLS)[:, None], np.arange(128)[None]
    m, s = row // 128, row % 128
    ax, ay, bx, by, cx, cy = s // 16, s % 16, m // 3, m % 3, lane // 8, lane % 8
    one = (ax * bx * 16 + ay * by * 8 + 0 * lane) * (2 * np.pi / NG)
    two = (cx * (ax + 8 * bx) + cy * (ay + 16 * by)) * (2 * np.pi / NG)
    return np.stack([np.cos(one), -np.sin(one), np.cos(two), -np.sin(two)]).astype(np.float32)


def signed(k):
    return jnp.where(k < NG // 2, k, k - NG).astype(F32)


def top_hat(freq_x, freq_y, freq_z):
    radial = jnp.sqrt(freq_x * freq_x + freq_y * freq_y + freq_z * freq_z) * (2.0 * jnp.pi * RADIUS / NG)
    safe = jnp.where(radial > 0, radial, 1.0)
    value = 3.0 * (jnp.sin(safe) - safe * jnp.cos(safe)) / (safe * safe * safe)
    return jnp.where(radial > 0, value, 1.0)


def call(body, out_shape, args, scratch, spaces=None, flops=0, nbytes=0, name=None, **params):
    spaces = spaces or [VMEM] * len(args)
    outs = jax.tree.map(lambda _: pl.BlockSpec(memory_space=VMEM), out_shape)
    return pl.pallas_call(
        body,
        out_shape=out_shape,
        in_specs=[pl.BlockSpec(memory_space=s) for s in spaces],
        out_specs=outs,
        scratch_shapes=scratch,
        compiler_params=pltpu.CompilerParams(vmem_limit_bytes=LIMIT, **params),
        cost_estimate=pl.CostEstimate(flops=flops, bytes_accessed=nbytes, transcendentals=0),
        name=name,
    )(*args)


def prep_body(ph_ref, cell_ref, count_row, own_row, out_ref):
    lane = lax.broadcasted_iota(jnp.int32, (32, SLOTS), 1)
    first = lax.broadcasted_iota(jnp.int32, (32, 32), 0)
    second = lax.broadcasted_iota(jnp.int32, (32, 32), 1)

    def column(row):
        spread = jnp.where(first == second, row.astype(F32), 0.0)
        return jnp.sum(spread, axis=1, keepdims=True).astype(jnp.int32)

    live = lane < column(count_row[...])
    w = jnp.where(live, ph_ref[...], 0.0)
    cell = jnp.where(live, cell_ref[...], 0)
    column_of = cell // NG
    gz = cell - column_of * NG
    gx = column_of // 24
    gy = column_of - gx * 24
    chunk = (gz >> 7) * 9 + (gx >> 4) * 3 + (gy >> 3)
    spot = ((chunk * 128 + (gx & 15) * 8 + (gy & 7)) * 128 + (gz & 127)).astype(F32)
    same = (column(own_row[...]) == own_row[...]) & (first < second)
    rank = jnp.sum(jnp.where(same, 1.0, 0.0), axis=0, keepdims=True).astype(jnp.int32)
    place = own_row[...] * (2 * CAP) + rank
    rows = lax.broadcasted_iota(jnp.int32, (DEV, 32), 0)
    total = jnp.zeros((DEV, SLOTS), F32)
    for values, shift in ((w, 0), (spot, CAP)):
        hot = jnp.where(rows == place + shift, 1.0, 0.0).astype(BF16)
        hi = values.astype(BF16)
        rest = values - hi.astype(F32)
        mid = rest.astype(BF16)
        low = (rest - mid.astype(F32)).astype(BF16)
        total = total + ((mm(hot, hi, NN) + mm(hot, mid, NN)) + mm(hot, low, NN))
    out_ref[...] = total.reshape(16, 2 * CAP, SLOTS)


def density_body(dens, t0h, t0l, t1h, t1l, x0, y1, gh, gl):
    for m in range(9):
        xh, lh = m // 3, m % 3
        rows = [dens[(16 * xh + xl) * 24 + 8 * lh : (16 * xh + xl) * 24 + 8 * lh + 8, :] for xl in range(16)]
        hi, lo = cut(jnp.concatenate(rows, axis=0))
        gh[m * 128 : (m + 1) * 128, :] = hi
        gl[m * 128 : (m + 1) * 128, :] = lo
    res = mm3(t0h[...], t0l[...], gh[...], gl[...], NT)
    x0[:, 0, :CELLS] = res[:DEV]
    x0[:, 0, CELLS:] = res[DEV:]
    y1[...] = mm3(t1h[...], t1l[...], gh[...], gl[...], NT)


BUFS = 4
UNROLL = 8


def paint_body(got, t0h, t0l, t1h, t1l, y1, x12, b0, b1, b2, b3, fh, fl):
    bufs = (b0, b1, b2, b3)
    zero = jnp.zeros((128, 128), F32)

    def clear(i, carry):
        at = pl.multiple_of(i * 128, 128)
        for b in bufs:
            b[pl.ds(at, 128), :] = zero
        return carry

    lax.fori_loop(0, 27, clear, 0)
    lane = lax.broadcasted_iota(jnp.int32, (1, 128), 1)

    def one_row(r, carry):
        src, slot = r >> 2, r & 3

        def more(jb):
            return (jb < SLOTS // UNROLL) & (got[src, slot, jnp.minimum(jb * UNROLL, SLOTS - 1)] > 0.0)

        def step(jb):
            for u in range(UNROLL):
                j = jb * UNROLL + u
                at = got[src, CAP + slot, j].astype(jnp.int32)
                b = bufs[u % BUFS]
                row = lax.shift_right_logical(at, 7)
                here = lane == lax.bitwise_and(at, 127)
                b[pl.ds(row, 1), :] = b[pl.ds(row, 1), :] + jnp.where(here, got[src, slot, j], 0.0)
            return jb + 1

        lax.while_loop(more, step, 0)
        return carry

    lax.fori_loop(0, 16 * CAP, one_row, 0)
    for m in range(9):
        for zc in range(3):
            at = (zc * 9 + m) * 128
            v = (b0[at : at + 128, :] + b1[at : at + 128, :]) + (b2[at : at + 128, :] + b3[at : at + 128, :])
            hi, lo = cut(v)
            fh[m * 128 : (m + 1) * 128, zc * 128 : (zc + 1) * 128] = hi
            fl[m * 128 : (m + 1) * 128, zc * 128 : (zc + 1) * 128] = lo
    part = mm3(t1h[...], t1l[...], fh[...], fl[...], NT)
    for c in range(2):
        x12[:TAIL, 0, c * CELLS : (c + 1) * CELLS] = y1[c * HEAD : c * HEAD + TAIL, :]
        x12[TAIL:HEAD, 0, c * CELLS : (c + 1) * CELLS] = (
            y1[c * HEAD + TAIL : (c + 1) * HEAD, :] + part[c * HEAD : c * HEAD + HEAD - TAIL]
        )
        x12[HEAD:, 0, c * CELLS : (c + 1) * CELLS] = part[c * HEAD + HEAD - TAIL : (c + 1) * HEAD]
    res = mm3(t0h[...], t0l[...], fh[...], fl[...], NT)
    x12[:, 0, PLANE : PLANE + CELLS] = res[:DEV]
    x12[:, 0, PLANE + CELLS :] = res[DEV:]


ROOT = 0.8660254037844386


def three(a, b, c, inverse):
    tr, ti = b[0] + c[0], b[1] + c[1]
    dr, di = ROOT * (b[0] - c[0]), ROOT * (b[1] - c[1])
    er, ei = a[0] - 0.5 * tr, a[1] - 0.5 * ti
    one, two = (er + di, ei - dr), (er - di, ei + dr)
    return (a[0] + tr, a[1] + ti), *((two, one) if inverse else (one, two))


def nine(v, inverse):
    v = list(v)
    for x in range(3):
        v[3 * x : 3 * x + 3] = three(*v[3 * x : 3 * x + 3], inverse)
    for y in range(3):
        v[y], v[y + 3], v[y + 6] = three(v[y], v[y + 3], v[y + 6], inverse)
    return v


def turn(v, c, s):
    return v[0] * c - v[1] * s, v[0] * s + v[1] * c


RB = 16
MESH = pl.DeviceIdType.MESH


def coords():
    px, py = lax.axis_index("px"), lax.axis_index("py")
    return px & 3, ((py >> 1) & 1) * 2 + (px >> 2), py >> 2, py & 1


def partner(t):
    x, y, z, core = coords()
    u = (t * 101) & 127
    sign = 1 - 2 * core
    x2 = (x + sign * ((u >> 1) & 3)) & 3
    y2 = (y + sign * ((u >> 3) & 3)) & 3
    z2 = (z + sign * ((u >> 5) & 3)) & 3
    return (y2 & 1) * 4 + x2, z2 * 4 + (y2 >> 1) * 2 + ((core + u) & 1)


def everyone(body):
    def step(t, carry):
        body(*partner(t))
        return carry

    lax.fori_loop(1, DEV, step, 0)


def fill_window(me, win):
    second = jnp.where(me < 63, 129 + me, jnp.where(me == 63, 0, jnp.where(me == 64, NG // 2, 64 + me)))
    lane = lax.broadcasted_iota(jnp.int32, (RB, 128), 1)
    sub = lax.broadcasted_iota(jnp.int32, (RB, 128), 0)
    for which, k in ((0, me + 1), (1, second)):
        scale = jnp.where((k == 0) | (k == NG // 2), 1.0, 2.0) / float(NG) ** 3
        fz = signed(k)

        def step(i, carry):
            m, r = i // (DEV // RB), i % (DEV // RB)
            s = sub + r * RB
            bx = m // 3
            kx = (s >> 4) + 8 * bx + 24 * (lane >> 3)
            ky = (s & 15) + 16 * (m - 3 * bx) + 48 * (lane & 7)
            value = top_hat(signed(kx), signed(ky), fz) * scale
            win[which, pl.ds(pl.multiple_of(i * RB, RB), RB), :] = value
            return carry

        lax.fori_loop(0, CELLS // RB, step, 0)


def planes_body(
    x0, x12, tw_hbm, ah, al, bh, bl, ch, cl, dh, dl, out,
    xs, ys, win, tw, wide, tall, uh, ul, vh, vl, sx, rx, sy, ry, own, sl,
):
    px, py = lax.axis_index("px"), lax.axis_index("py")
    me = px * 16 + py
    loads = [
        pltpu.make_async_copy(x0, xs.at[0], sl.at[0]),
        pltpu.make_async_copy(tw_hbm, tw, sl.at[1]),
    ]
    for q in range(2):
        mine = x12.at[me, :, pl.ds(q * PLANE, PLANE)]
        loads.append(pltpu.make_async_copy(mine, xs.at[q + 1, me], sl.at[2 + q]))
    for c in loads:
        c.start()
    barrier = pltpu.get_barrier_semaphore()
    everyone(lambda a, b: pl.semaphore_signal(barrier, inc=1, device_id=(a, b), device_id_type=MESH))
    pl.semaphore_wait(barrier, DEV - 1)
    for q in range(2):
        everyone(
            lambda a, b: pltpu.make_async_remote_copy(
                src_ref=x12.at[a * 16 + b, :, pl.ds(q * PLANE, PLANE)],
                dst_ref=xs.at[q + 1, me],
                send_sem=sx.at[q],
                recv_sem=rx.at[q],
                device_id=(a, b),
                device_id_type=MESH,
            ).start()
        )
    fill_window(me, win)
    for c in loads:
        c.wait()

    def one_plane(p, carry):
        @pl.when(p > 0)
        def _():
            part = xs.at[p, pl.ds(0, DEV - 1)]
            pltpu.make_async_copy(part, part, rx.at[p - 1]).wait()

        for c in range(2):
            wide[c * DEV : (c + 1) * DEV, :] = xs[p, :, 0, c * CELLS : (c + 1) * CELLS]
        hi, lo = cut(wide[...])
        wide[...] = mm3(ah[...], al[...], hi, lo)

        def forward(i, inner):
            r = pl.multiple_of(i * RB, RB)
            v = []
            for m in range(9):
                cols = slice(m * 128, (m + 1) * 128)
                t = pl.ds(m * 128 + r, RB)
                u = (wide[pl.ds(r, RB), cols], wide[pl.ds(DEV + r, RB), cols])
                v.append(turn(u, tw[0, t, :], tw[1, t, :]))
            for m, u in enumerate(nine(v, False)):
                t = pl.ds(m * 128 + r, RB)
                for c, part in enumerate(turn(u, tw[2, t, :], tw[3, t, :])):
                    hi, lo = cut(part)
                    uh[t, c * 128 : (c + 1) * 128] = hi
                    ul[t, c * 128 : (c + 1) * 128] = lo
            return inner

        lax.fori_loop(0, DEV // RB, forward, 0)
        mid = mm3(uh[...], ul[...], ch[...], cl[...])
        this = win[p & 1]
        for c in range(2):
            hi, lo = cut(mid[:, c * 128 : (c + 1) * 128] * this)
            uh[:, c * 128 : (c + 1) * 128] = hi
            ul[:, c * 128 : (c + 1) * 128] = lo
        tall[...] = mm3(uh[...], ul[...], dh[...], dl[...])

        def backward(i, inner):
            r = pl.multiple_of(i * RB, RB)
            v = []
            for m in range(9):
                t = pl.ds(m * 128 + r, RB)
                v.append(turn((tall[t, :128], tall[t, 128:]), tw[2, t, :], -tw[3, t, :]))
            for m, u in enumerate(nine(v, True)):
                t = pl.ds(m * 128 + r, RB)
                cols = slice(m * 128, (m + 1) * 128)
                for c, part in enumerate(turn(u, tw[0, t, :], -tw[1, t, :])):
                    hi, lo = cut(part)
                    vh[pl.ds(c * DEV + r, RB), cols] = hi
                    vl[pl.ds(c * DEV + r, RB), cols] = lo
            return inner

        lax.fori_loop(0, DEV // RB, backward, 0)
        back = mm3(bh[...], bl[...], vh[...], vl[...])
        for c in range(2):
            ys[p, :, 0, c * CELLS : (c + 1) * CELLS] = back[c * DEV : (c + 1) * DEV]
        mine = pltpu.make_async_copy(ys.at[p, me], out.at[p, me], own)
        mine.start()
        mine.wait()
        everyone(
            lambda a, b: pltpu.make_async_remote_copy(
                src_ref=ys.at[p, a * 16 + b],
                dst_ref=out.at[p, me],
                send_sem=sy.at[p],
                recv_sem=ry.at[p],
                device_id=(a, b),
                device_id_type=MESH,
            ).start()
        )
        return carry

    lax.fori_loop(0, 3, one_plane, 0)
    for q in range(2):
        part = x12.at[pl.ds(0, DEV - 1), :, pl.ds(q * PLANE, PLANE)]
        pltpu.make_async_copy(part, part, sx.at[q]).wait()
    for p in range(3):
        part = ys.at[p, pl.ds(0, DEV - 1)]
        pltpu.make_async_copy(part, part, sy.at[p]).wait()
        part = out.at[p, pl.ds(0, DEV - 1)]
        pltpu.make_async_copy(part, part, ry.at[p]).wait()


def last_body(r, gth, gtl, fth, ftl, out, stack, ga, fa):
    for c in range(2):
        cols = slice(c * CELLS, (c + 1) * CELLS)
        stack[c * DEV : (c + 1) * DEV, :] = r[0, :, 0, cols]
        stack[2 * DEV + c * HEAD : 2 * DEV + (c + 1) * HEAD, :] = r[1, :HEAD, 0, cols]
    hi, lo = cut(stack[...])
    ga[...] = mm3(gth[...], gtl[...], hi, lo)
    for c in range(2):
        cols = slice(c * CELLS, (c + 1) * CELLS)
        stack[c * DEV : (c + 1) * DEV, :] = r[2, :, 0, cols]
        stack[2 * DEV + c * HEAD : 2 * DEV + (c + 1) * HEAD, :] = r[1, TAIL:, 0, cols]
    hi, lo = cut(stack[...])
    fa[...] = mm3(fth[...], ftl[...], hi, lo)
    for m in range(9):
        xh, lh = m // 3, m % 3
        cols = slice(m * 128, (m + 1) * 128)
        frac = jnp.clip(fa[:, cols] / jnp.maximum(ga[:, cols], 0.5), 0.0, 1.0)
        turned = frac.T
        for xl in range(16):
            at = (16 * xh + xl) * 24 + 8 * lh
            out[at : at + 8, :] = turned[xl * 8 : xl * 8 + 8, :]


def sds(*shape, dtype=F32):
    return jax.ShapeDtypeStruct(shape, dtype)


def exchange(a):
    return lax.all_to_all(a, ("px", "py"), split_axis=0, concat_axis=0, tiled=True)


def planes(x0, x12, tw, mats):
    dma = pltpu.SemaphoreType.DMA
    plane = (DEV, 1, PLANE)
    return pl.pallas_call(
        planes_body,
        out_shape=sds(3, *plane),
        in_specs=[pl.BlockSpec(memory_space=pl.ANY)] * 3 + [pl.BlockSpec(memory_space=VMEM)] * 8,
        out_specs=pl.BlockSpec(memory_space=pl.ANY),
        scratch_shapes=[
            VMEM((3, *plane), F32),
            VMEM((3, *plane), F32),
            VMEM((2, CELLS, 128), F32),
            VMEM((4, CELLS, 128), F32),
            VMEM((256, CELLS), F32),
            VMEM((CELLS, 256), F32),
            VMEM((CELLS, 256), BF16),
            VMEM((CELLS, 256), BF16),
            VMEM((256, CELLS), BF16),
            VMEM((256, CELLS), BF16),
            dma((2,)),
            dma((2,)),
            dma((3,)),
            dma((3,)),
            dma,
            dma((4,)),
        ],
        compiler_params=pltpu.CompilerParams(vmem_limit_bytes=LIMIT, collective_id=1, has_side_effects=True),
        cost_estimate=pl.CostEstimate(flops=36 << 30, bytes_accessed=8 << 20, transcendentals=0),
        name="planes",
    )(x0, x12, tw, *mats)


def on_device(photons, halo_cells, halo_counts, owners, density):
    first, second_g, second_f = z_tables()
    t0 = [jnp.asarray(t) for t in cut_np(first)]
    t1g = [jnp.asarray(t) for t in cut_np(second_g)]
    t1f = [jnp.asarray(t) for t in cut_np(second_f)]
    back_g = [jnp.asarray(t) for t in cut_np(np.concatenate([first, second_g]).T)]
    back_f = [jnp.asarray(t) for t in cut_np(np.concatenate([first, second_f]).T)]
    mats = []
    for m in (row_matrix(1), row_matrix(-1), lane_matrix(1), lane_matrix(-1)):
        mats += [jnp.asarray(t) for t in cut_np(m)]

    send = call(
        prep_body,
        sds(16, 2 * CAP, SLOTS),
        (photons, halo_cells, halo_counts.reshape(1, 32), owners.reshape(1, 32)),
        [],
        flops=1 << 20,
        nbytes=1 << 17,
        name="prep",
    )
    got = lax.all_to_all(send, "py", split_axis=0, concat_axis=0, tiled=True)
    x0, y1 = call(
        density_body,
        (sds(DEV, 1, PLANE), sds(2 * HEAD, CELLS)),
        (density.reshape(CELLS, NG), *t0, *t1g),
        [VMEM((CELLS, NG), BF16)] * 2,
        flops=6 * 400 * NG * CELLS,
        nbytes=4 << 20,
        name="density",
    )
    x0 = exchange(x0)
    x12 = call(
        paint_body,
        sds(DEV, 1, 2 * PLANE),
        (got, *t0, *t1f, y1),
        [VMEM((3 * CELLS, 128), F32)] * BUFS + [VMEM((CELLS, NG), BF16)] * 2,
        spaces=[SMEM] + [VMEM] * 5,
        flops=6 * 400 * NG * CELLS * 3,
        nbytes=4 << 20,
        name="paint",
    )
    r = planes(x0, x12, jnp.asarray(twiddles()), mats)
    out = call(
        last_body,
        sds(CELLS, NG),
        (r, *back_g, *back_f),
        [VMEM((400, CELLS), F32), VMEM((NG, CELLS), F32), VMEM((NG, CELLS), F32)],
        flops=6 * 2 * 400 * NG * CELLS,
        nbytes=6 << 20,
        name="last",
    )
    return out.reshape(48, 24, NG)


def solution(mesh):
    placed = (
        P(("px", "py"), None),
        P(("px", "py"), None),
        P(("px", "py")),
        P(("px", "py"), None),
        P("px", "py", None),
    )
    return jax.shard_map(
        on_device, mesh=mesh, in_specs=placed, out_specs=P("px", "py", None), check_vma=False
    )
```

```python
import functools

import jax
import jax.numpy as jnp
import numpy as np
from jax import lax
from jax.experimental import pallas as pl
from jax.experimental.pallas import tpu as pltpu
from jax.sharding import PartitionSpec as P

NG = 384
SLOTS = 128
CAP = 4
RADIUS = 20
DEV = 128
CELLS = 1152
PLANE = 2 * CELLS
HALF = 3 * CELLS
LIMIT = 60 * 1024 * 1024
F32 = jnp.float32
BF16 = jnp.bfloat16
VMEM = pltpu.VMEM
SMEM = pltpu.SMEM


def cut(v):
    hi = v.astype(BF16)
    return hi, (v - hi.astype(F32)).astype(BF16)


def cut_np(v):
    v = np.asarray(v, np.float32)
    hi = v.astype(jnp.bfloat16)
    lo = (v - hi.astype(np.float32)).astype(jnp.bfloat16)
    return hi, lo


NN = (((1,), (0,)), ((), ()))
NT = (((1,), (1,)), ((), ()))


def mm(a, b, dims):
    return lax.dot_general(a, b, dims, preferred_element_type=F32)


def mm3(ah, al, bh, bl, dims=NN):
    return mm(ah, bh, dims) + (mm(ah, bl, dims) + mm(al, bh, dims))


def z_table():
    k = np.arange(1, NG // 2)[:, None] * np.arange(NG)[None]
    angle = 2 * np.pi * (k % NG) / NG
    c, s = np.cos(angle), np.sin(angle)
    ends = np.stack([np.ones(NG), 1.0 - 2.0 * (np.arange(NG) % 2)])
    return np.concatenate([c[:DEV], s[:DEV], c[DEV:], s[DEV:], ends])


def stacked(v, axis):
    hi, lo = cut_np(v)
    return jnp.asarray(np.concatenate([hi, hi, lo], axis=axis))


def mix(left, right):
    i = np.arange(left * right)
    a, b = i // right, i % right
    ph = -2j * np.pi * (np.outer(a, a) / left + np.outer(b, b) / right)
    return np.exp(ph)


def row_matrix(sign):
    m = mix(8, 16)
    re, im = m.real, sign * m.imag
    return np.block([[re, -im], [im, re]])


def lane_matrix(sign):
    m = mix(16, 8)
    re, im = m.real, sign * m.imag
    return np.block([[re, im], [-im, re]])


def twiddles():
    row, lane = np.arange(CELLS)[:, None], np.arange(128)[None]
    m, s = row // 128, row % 128
    ax, ay, bx, by, cx, cy = s // 16, s % 16, m // 3, m % 3, lane // 8, lane % 8
    one = (ax * bx * 16 + ay * by * 8 + 0 * lane) * (2 * np.pi / NG)
    two = (cx * (ax + 8 * bx) + cy * (ay + 16 * by)) * (2 * np.pi / NG)
    return np.stack([np.cos(one), -np.sin(one), np.cos(two), -np.sin(two)]).astype(np.float32)


def signed(k):
    return jnp.where(k < NG // 2, k, k - NG).astype(F32)


def top_hat(freq_x, freq_y, freq_z):
    radial = jnp.sqrt(freq_x * freq_x + freq_y * freq_y + freq_z * freq_z) * (2.0 * jnp.pi * RADIUS / NG)
    safe = jnp.where(radial > 0, radial, 1.0)
    value = 3.0 * (jnp.sin(safe) - safe * jnp.cos(safe)) / (safe * safe * safe)
    return jnp.where(radial > 0, value, 1.0)


def call(body, out_shape, args, scratch, spaces=None, flops=0, nbytes=0, name=None, **params):
    spaces = spaces or [VMEM] * len(args)
    outs = jax.tree.map(lambda _: pl.BlockSpec(memory_space=VMEM), out_shape)
    return pl.pallas_call(
        body,
        out_shape=out_shape,
        in_specs=[pl.BlockSpec(memory_space=s) for s in spaces],
        out_specs=outs,
        scratch_shapes=scratch,
        compiler_params=pltpu.CompilerParams(vmem_limit_bytes=LIMIT, **params),
        cost_estimate=pl.CostEstimate(flops=flops, bytes_accessed=nbytes, transcendentals=0),
        name=name,
    )(*args)


def prep_body(ph_ref, cell_ref, count_row, own_row, out_ref):
    lane = lax.broadcasted_iota(jnp.int32, (32, SLOTS), 1)
    first = lax.broadcasted_iota(jnp.int32, (32, 32), 0)
    second = lax.broadcasted_iota(jnp.int32, (32, 32), 1)

    def column(row):
        spread = jnp.where(first == second, row.astype(F32), 0.0)
        return jnp.sum(spread, axis=1, keepdims=True).astype(jnp.int32)

    live = lane < column(count_row[...])
    w = jnp.where(live, ph_ref[...], 0.0)
    cell = jnp.where(live, cell_ref[...], 0)
    column_of = cell // NG
    gz = cell - column_of * NG
    gx = column_of // 24
    gy = column_of - gx * 24
    chunk = (gz >> 7) * 9 + (gx >> 4) * 3 + (gy >> 3)
    spot = ((chunk * 128 + (gx & 15) * 8 + (gy & 7)) * 128 + (gz & 127)).astype(F32)
    same = (column(own_row[...]) == own_row[...]) & (first < second)
    rank = jnp.sum(jnp.where(same, 1.0, 0.0), axis=0, keepdims=True).astype(jnp.int32)
    place = own_row[...] * (2 * CAP) + rank
    rows = lax.broadcasted_iota(jnp.int32, (DEV, 32), 0)
    total = jnp.zeros((DEV, SLOTS), F32)
    for values, shift in ((w, 0), (spot, CAP)):
        hot = jnp.where(rows == place + shift, 1.0, 0.0).astype(BF16)
        hi = values.astype(BF16)
        rest = values - hi.astype(F32)
        mid = rest.astype(BF16)
        low = (rest - mid.astype(F32)).astype(BF16)
        total = total + ((mm(hot, hi, NN) + mm(hot, mid, NN)) + mm(hot, low, NN))
    out_ref[...] = total.reshape(16, 2 * CAP, SLOTS)


def density_body(dens, table, xg, g3):
    for m in range(9):
        xh, lh = m // 3, m % 3
        rows = [dens[(16 * xh + xl) * 24 + 8 * lh : (16 * xh + xl) * 24 + 8 * lh + 8, :] for xl in range(16)]
        hi, lo = cut(jnp.concatenate(rows, axis=0))
        at = slice(m * 128, (m + 1) * 128)
        g3[at, :NG] = hi
        g3[at, NG : 2 * NG] = lo
        g3[at, 2 * NG :] = hi
    res = mm(table[...], g3[...], NT)
    for c in range(3):
        xg[:, 0, c * CELLS : (c + 1) * CELLS] = res[c * DEV : (c + 1) * DEV]


BUFS = 2
UNROLL = 16


def paint_body(got, table, xf, b0, b1, f3, iv, pv, cells, weights, sem):
    bufs = (b0, b1)
    iv[...] = got[:, CAP:].reshape(16 * CAP, SLOTS).astype(jnp.int32)
    pv[...] = got[:, :CAP].reshape(16 * CAP, SLOTS)
    loads = [pltpu.make_async_copy(iv, cells, sem.at[0]), pltpu.make_async_copy(pv, weights, sem.at[1])]
    for c in loads:
        c.start()
    zero = jnp.zeros((128, 128), F32)

    def clear(i, carry):
        at = pl.multiple_of(i * 128, 128)
        for b in bufs:
            b[pl.ds(at, 128), :] = zero
        return carry

    lax.fori_loop(0, 27, clear, 0)
    for c in loads:
        c.wait()
    lane = lax.broadcasted_iota(jnp.int32, (1, 128), 1)

    def one_row(r, carry):
        def more(jb):
            return (jb < SLOTS // UNROLL) & (weights[r, jnp.minimum(jb * UNROLL, SLOTS - 1)] > 0.0)

        def step(jb):
            for u in range(UNROLL):
                j = jb * UNROLL + u
                at = cells[r, j]
                b = bufs[u % BUFS]
                row = lax.shift_right_logical(at, 7)
                here = lane == lax.bitwise_and(at, 127)
                b[pl.ds(row, 1), :] = b[pl.ds(row, 1), :] + jnp.where(here, weights[r, j], 0.0)
            return jb + 1

        lax.while_loop(more, step, 0)
        return carry

    lax.fori_loop(0, 16 * CAP, one_row, 0)
    for m in range(9):
        for zc in range(3):
            at = (zc * 9 + m) * 128
            hi, lo = cut(b0[at : at + 128, :] + b1[at : at + 128, :])
            rows = slice(m * 128, (m + 1) * 128)
            f3[rows, zc * 128 : (zc + 1) * 128] = hi
            f3[rows, NG + zc * 128 : NG + (zc + 1) * 128] = lo
            f3[rows, 2 * NG + zc * 128 : 2 * NG + (zc + 1) * 128] = hi
    res = mm(table[...], f3[...], NT)
    xf[0, :, 0, :] = res[2 * DEV :]
    xf[1, :, 0, :] = res[:DEV]
    xf[2, :, 0, :] = res[DEV : 2 * DEV]


ROOT = 0.8660254037844386


def three(a, b, c, inverse):
    tr, ti = b[0] + c[0], b[1] + c[1]
    dr, di = ROOT * (b[0] - c[0]), ROOT * (b[1] - c[1])
    er, ei = a[0] - 0.5 * tr, a[1] - 0.5 * ti
    one, two = (er + di, ei - dr), (er - di, ei + dr)
    return (a[0] + tr, a[1] + ti), *((two, one) if inverse else (one, two))


def nine(v, inverse):
    v = list(v)
    for x in range(3):
        v[3 * x : 3 * x + 3] = three(*v[3 * x : 3 * x + 3], inverse)
    for y in range(3):
        v[y], v[y + 3], v[y + 6] = three(v[y], v[y + 3], v[y + 6], inverse)
    return v


def turn(v, c, s):
    return v[0] * c - v[1] * s, v[0] * s + v[1] * c


RB = 16
MESH = pl.DeviceIdType.MESH


def coords():
    px, py = lax.axis_index("px"), lax.axis_index("py")
    return px & 3, ((py >> 1) & 1) * 2 + (px >> 2), py >> 2, py & 1


def partner(t):
    x, y, z, core = coords()
    u = (t * 101) & 127
    sign = 1 - 2 * core
    x2 = (x + sign * ((u >> 1) & 3)) & 3
    y2 = (y + sign * ((u >> 3) & 3)) & 3
    z2 = (z + sign * ((u >> 5) & 3)) & 3
    return (y2 & 1) * 4 + x2, z2 * 4 + (y2 >> 1) * 2 + ((core + u) & 1)


def everyone(body):
    def step(t, carry):
        body(*partner(t))
        return carry

    lax.fori_loop(1, DEV, step, 0)


def fill_window(k, which, win):
    lane = lax.broadcasted_iota(jnp.int32, (RB, 128), 1)
    sub = lax.broadcasted_iota(jnp.int32, (RB, 128), 0)
    scale = jnp.where((k == 0) | (k == NG // 2), 1.0, 2.0) / float(NG) ** 3
    fz = signed(k)

    def step(i, carry):
        m, r = i // (DEV // RB), i % (DEV // RB)
        s = sub + r * RB
        bx = m // 3
        kx = (s >> 4) + 8 * bx + 24 * (lane >> 3)
        ky = (s & 15) + 16 * (m - 3 * bx) + 48 * (lane & 7)
        value = top_hat(signed(kx), signed(ky), fz) * scale
        win[which, pl.ds(pl.multiple_of(i * RB, RB), RB), :] = value
        return carry

    lax.fori_loop(0, CELLS // RB, step, 0)


def planes_body(
    xg, xf, tw_hbm, ah, al, bh, bl, ch, cl, dh, dl, out,
    xs, ys, win, tw, wide, tall, uh, ul, vh, vl, sx, rx, sy, ry, own, sl,
):
    px, py = lax.axis_index("px"), lax.axis_index("py")
    me = px * 16 + py
    loads = [pltpu.make_async_copy(tw_hbm, tw, sl.at[0])]
    for c in range(3):
        loads.append(pltpu.make_async_copy(xg.at[:, :, pl.ds(c * CELLS, CELLS)], xs.at[c], sl.at[1 + c]))
        loads.append(pltpu.make_async_copy(xf.at[c, me], xs.at[3 + c, me], sl.at[4 + c]))
    for c in loads:
        c.start()
    barrier = pltpu.get_barrier_semaphore()
    everyone(lambda a, b: pl.semaphore_signal(barrier, inc=1, device_id=(a, b), device_id_type=MESH))
    pl.semaphore_wait(barrier, DEV - 1)
    pieces = ((0, 1), (1, 2))
    for q, (start, size) in enumerate(pieces):
        everyone(
            lambda a, b: pltpu.make_async_remote_copy(
                src_ref=xf.at[pl.ds(start, size), a * 16 + b],
                dst_ref=xs.at[pl.ds(3 + start, size), me],
                send_sem=sx.at[q],
                recv_sem=rx.at[q],
                device_id=(a, b),
                device_id_type=MESH,
            ).start()
        )
    fill_window(me + 1, 0, win)
    for c in loads:
        c.wait()

    def one_plane(p, carry):
        for q, (start, size) in enumerate(pieces):

            @pl.when(p == q + 1)
            def _():
                part = xs.at[pl.ds(3 + start, size), pl.ds(0, DEV - 1)]
                pltpu.make_async_copy(part, part, rx.at[q]).wait()

        for c in range(2):
            wide[c * DEV : (c + 1) * DEV, :] = xs[2 * p + c, :, 0, :]
        hi, lo = cut(wide[...])
        wide[...] = mm3(ah[...], al[...], hi, lo)

        def forward(i, inner):
            r = pl.multiple_of(i * RB, RB)
            v = []
            for m in range(9):
                cols = slice(m * 128, (m + 1) * 128)
                t = pl.ds(m * 128 + r, RB)
                u = (wide[pl.ds(r, RB), cols], wide[pl.ds(DEV + r, RB), cols])
                v.append(turn(u, tw[0, t, :], tw[1, t, :]))
            for m, u in enumerate(nine(v, False)):
                t = pl.ds(m * 128 + r, RB)
                for c, part in enumerate(turn(u, tw[2, t, :], tw[3, t, :])):
                    hi, lo = cut(part)
                    uh[t, c * 128 : (c + 1) * 128] = hi
                    ul[t, c * 128 : (c + 1) * 128] = lo
            return inner

        lax.fori_loop(0, DEV // RB, forward, 0)
        mid = mm3(uh[...], ul[...], ch[...], cl[...])
        this = win[p & 1]
        for c in range(2):
            hi, lo = cut(mid[:, c * 128 : (c + 1) * 128] * this)
            uh[:, c * 128 : (c + 1) * 128] = hi
            ul[:, c * 128 : (c + 1) * 128] = lo
        tall[...] = mm3(uh[...], ul[...], dh[...], dl[...])

        def backward(i, inner):
            r = pl.multiple_of(i * RB, RB)
            v = []
            for m in range(9):
                t = pl.ds(m * 128 + r, RB)
                v.append(turn((tall[t, :128], tall[t, 128:]), tw[2, t, :], -tw[3, t, :]))
            for m, u in enumerate(nine(v, True)):
                t = pl.ds(m * 128 + r, RB)
                cols = slice(m * 128, (m + 1) * 128)
                for c, part in enumerate(turn(u, tw[0, t, :], -tw[1, t, :])):
                    hi, lo = cut(part)
                    vh[pl.ds(c * DEV + r, RB), cols] = hi
                    vl[pl.ds(c * DEV + r, RB), cols] = lo
            return inner

        lax.fori_loop(0, DEV // RB, backward, 0)
        back = mm3(bh[...], bl[...], vh[...], vl[...])
        for c in range(2):
            ys[p, :, 0, c * CELLS : (c + 1) * CELLS] = back[c * DEV : (c + 1) * DEV]
        mine = pltpu.make_async_copy(ys.at[p, me], out.at[p, me], own)
        mine.start()
        mine.wait()
        everyone(
            lambda a, b: pltpu.make_async_remote_copy(
                src_ref=ys.at[p, a * 16 + b],
                dst_ref=out.at[p, me],
                send_sem=sy.at[p],
                recv_sem=ry.at[p],
                device_id=(a, b),
                device_id_type=MESH,
            ).start()
        )

        @pl.when(p == 0)
        def _():
            second = jnp.where(me < 63, 129 + me, jnp.where(me < 126, 66 + me, (me - 126) * (NG // 2)))
            fill_window(second, 1, win)

        return carry

    lax.fori_loop(0, 3, one_plane, 0)
    for q, (start, size) in enumerate(pieces):
        part = xf.at[pl.ds(start, size), pl.ds(0, DEV - 1)]
        pltpu.make_async_copy(part, part, sx.at[q]).wait()
    for p in range(3):
        part = ys.at[p, pl.ds(0, DEV - 1)]
        pltpu.make_async_copy(part, part, sy.at[p]).wait()
        part = out.at[p, pl.ds(0, DEV - 1)]
        pltpu.make_async_copy(part, part, ry.at[p]).wait()


def last_body(r, table, out, stack, ga, fa):
    parts = (((0, 0), (0, 1), (1, 0)), ((2, 0), (2, 1), (1, 1)))
    for result, rows in zip((ga, fa), parts):
        for i, (p, c) in enumerate(rows):
            result[i * DEV : (i + 1) * DEV, :] = r[p, :, 0, c * CELLS : (c + 1) * CELLS]
        hi, lo = cut(result[...])
        stack[:NG, :] = hi
        stack[NG : 2 * NG, :] = lo
        stack[2 * NG :, :] = hi
        result[...] = mm(table[...], stack[...], NN)
    for m in range(9):
        xh, lh = m // 3, m % 3
        cols = slice(m * 128, (m + 1) * 128)
        frac = jnp.clip(fa[:, cols] / jnp.maximum(ga[:, cols], 0.5), 0.0, 1.0)
        turned = frac.T
        for xl in range(16):
            at = (16 * xh + xl) * 24 + 8 * lh
            out[at : at + 8, :] = turned[xl * 8 : xl * 8 + 8, :]


def sds(*shape, dtype=F32):
    return jax.ShapeDtypeStruct(shape, dtype)


def exchange(a):
    return lax.all_to_all(a, ("px", "py"), split_axis=0, concat_axis=0, tiled=True)


def planes(xg, xf, tw, mats):
    dma = pltpu.SemaphoreType.DMA
    plane = (DEV, 1, PLANE)
    return pl.pallas_call(
        planes_body,
        out_shape=sds(3, *plane),
        in_specs=[pl.BlockSpec(memory_space=pl.ANY)] * 3 + [pl.BlockSpec(memory_space=VMEM)] * 8,
        out_specs=pl.BlockSpec(memory_space=pl.ANY),
        scratch_shapes=[
            VMEM((6, DEV, 1, CELLS), F32),
            VMEM((3, *plane), F32),
            VMEM((2, CELLS, 128), F32),
            VMEM((4, CELLS, 128), F32),
            VMEM((256, CELLS), F32),
            VMEM((CELLS, 256), F32),
            VMEM((CELLS, 256), BF16),
            VMEM((CELLS, 256), BF16),
            VMEM((256, CELLS), BF16),
            VMEM((256, CELLS), BF16),
            dma((2,)),
            dma((2,)),
            dma((3,)),
            dma((3,)),
            dma,
            dma((7,)),
        ],
        compiler_params=pltpu.CompilerParams(vmem_limit_bytes=LIMIT, collective_id=1, has_side_effects=True),
        cost_estimate=pl.CostEstimate(flops=36 << 30, bytes_accessed=8 << 20, transcendentals=0),
        name="planes",
    )(xg, xf, tw, *mats)


def on_device(photons, halo_cells, halo_counts, owners, density):
    table = z_table()
    ahead, back = stacked(table, 1), stacked(table.T, 1)
    mats = []
    for m in (row_matrix(1), row_matrix(-1), lane_matrix(1), lane_matrix(-1)):
        mats += [jnp.asarray(t) for t in cut_np(m)]

    send = call(
        prep_body,
        sds(16, 2 * CAP, SLOTS),
        (photons, halo_cells, halo_counts.reshape(1, 32), owners.reshape(1, 32)),
        [],
        flops=1 << 20,
        nbytes=1 << 17,
        name="prep",
    )
    got = lax.all_to_all(send, "py", split_axis=0, concat_axis=0, tiled=True)
    xg = call(
        density_body,
        sds(DEV, 1, HALF),
        (density.reshape(CELLS, NG), ahead),
        [VMEM((CELLS, 3 * NG), BF16)],
        flops=6 * 400 * NG * CELLS,
        nbytes=4 << 20,
        name="density",
    )
    xg = exchange(xg)
    xf = call(
        paint_body,
        sds(3, DEV, 1, CELLS),
        (got, ahead),
        [VMEM((3 * CELLS, 128), F32)] * BUFS
        + [VMEM((CELLS, 3 * NG), BF16)]
        + [VMEM((16 * CAP, SLOTS), jnp.int32), VMEM((16 * CAP, SLOTS), F32)]
        + [SMEM((16 * CAP, SLOTS), jnp.int32), SMEM((16 * CAP, SLOTS), F32)]
        + [pltpu.SemaphoreType.DMA((2,))],
        flops=6 * 400 * NG * CELLS * 3,
        nbytes=4 << 20,
        name="paint",
    )
    r = planes(xg, xf, jnp.asarray(twiddles()), mats)
    out = call(
        last_body,
        sds(CELLS, NG),
        (r, back),
        [VMEM((3 * NG, CELLS), BF16), VMEM((NG, CELLS), F32), VMEM((NG, CELLS), F32)],
        flops=6 * 2 * 400 * NG * CELLS,
        nbytes=6 << 20,
        name="last",
    )
    return out.reshape(48, 24, NG)


def solution(mesh):
    placed = (
        P(("px", "py"), None),
        P(("px", "py"), None),
        P(("px", "py")),
        P(("px", "py"), None),
        P("px", "py", None),
    )
    return jax.shard_map(
        on_device, mesh=mesh, in_specs=placed, out_specs=P("px", "py", None), check_vma=False
    )
```

```python
import functools

import jax
import jax.numpy as jnp
import numpy as np
from jax import lax
from jax.experimental import pallas as pl
from jax.experimental.pallas import tpu as pltpu
from jax.sharding import PartitionSpec as P

NG = 384
SLOTS = 128
CAP = 4
RADIUS = 20
DEV = 128
CELLS = 1152
PLANE = 2 * CELLS
HALF = 3 * CELLS
LIMIT = 60 * 1024 * 1024
F32 = jnp.float32
BF16 = jnp.bfloat16
VMEM = pltpu.VMEM
MESH = pl.DeviceIdType.MESH


def cut(v):
    hi = v.astype(BF16)
    return hi, (v - hi.astype(F32)).astype(BF16)


def cut_np(v):
    v = np.asarray(v, np.float32)
    hi = v.astype(jnp.bfloat16)
    lo = (v - hi.astype(np.float32)).astype(jnp.bfloat16)
    return hi, lo


NN = (((1,), (0,)), ((), ()))
NT = (((1,), (1,)), ((), ()))


def mm(a, b, dims):
    return lax.dot_general(a, b, dims, preferred_element_type=F32)


def mm3(ah, al, bh, bl, dims=NN):
    return mm(ah, bh, dims) + (mm(ah, bl, dims) + mm(al, bh, dims))


def z_table():
    k = np.arange(1, NG // 2)[:, None] * np.arange(NG)[None]
    angle = 2 * np.pi * (k % NG) / NG
    c, s = np.cos(angle), np.sin(angle)
    ends = np.stack([np.ones(NG), 1.0 - 2.0 * (np.arange(NG) % 2)])
    return np.concatenate([c[:DEV], s[:DEV], c[DEV:], s[DEV:], ends])


def stacked(v, axis):
    hi, lo = cut_np(v)
    return jnp.asarray(np.concatenate([hi, hi, lo], axis=axis))


def mix(left, right):
    i = np.arange(left * right)
    a, b = i // right, i % right
    ph = -2j * np.pi * (np.outer(a, a) / left + np.outer(b, b) / right)
    return np.exp(ph)


def row_matrix(sign):
    m = mix(8, 16)
    re, im = m.real, sign * m.imag
    return np.block([[re, -im], [im, re]])


def lane_matrix(sign):
    m = mix(16, 8)
    re, im = m.real, sign * m.imag
    return np.block([[re, im], [-im, re]])


def twiddles():
    row, lane = np.arange(CELLS)[:, None], np.arange(128)[None]
    m, s = row // 128, row % 128
    ax, ay, bx, by, cx, cy = s // 16, s % 16, m // 3, m % 3, lane // 8, lane % 8
    one = (ax * bx * 16 + ay * by * 8 + 0 * lane) * (2 * np.pi / NG)
    two = (cx * (ax + 8 * bx) + cy * (ay + 16 * by)) * (2 * np.pi / NG)
    return np.stack([np.cos(one), -np.sin(one), np.cos(two), -np.sin(two)]).astype(np.float32)


def signed(k):
    return jnp.where(k < NG // 2, k, k - NG).astype(F32)


def top_hat(freq_x, freq_y, freq_z):
    radial = jnp.sqrt(freq_x * freq_x + freq_y * freq_y + freq_z * freq_z) * (2.0 * jnp.pi * RADIUS / NG)
    safe = jnp.where(radial > 0, radial, 1.0)
    value = 3.0 * (jnp.sin(safe) - safe * jnp.cos(safe)) / (safe * safe * safe)
    return jnp.where(radial > 0, value, 1.0)


def pack(photons, cells, counts, owned):
    lane = lax.broadcasted_iota(jnp.int32, (32, SLOTS), 1)
    first = lax.broadcasted_iota(jnp.int32, (32, 32), 0)
    second = lax.broadcasted_iota(jnp.int32, (32, 32), 1)

    def column(row):
        spread = jnp.where(first == second, row.astype(F32), 0.0)
        return jnp.sum(spread, axis=1, keepdims=True).astype(jnp.int32)

    live = lane < column(counts)
    w = jnp.where(live, photons, 0.0)
    cell = jnp.where(live, cells, 0)
    column_of = cell // NG
    gz = cell - column_of * NG
    gx = column_of // 24
    gy = column_of - gx * 24
    place_in = ((gx >> 4) * 3 + (gy >> 3)) * 128 + (gx & 15) * 8 + (gy & 7)
    spot = (place_in * 512 + gz).astype(F32)
    same = (column(owned) == owned) & (first < second)
    rank = jnp.sum(jnp.where(same, 1.0, 0.0), axis=0, keepdims=True).astype(jnp.int32)
    place = owned * (2 * CAP) + rank
    rows = lax.broadcasted_iota(jnp.int32, (DEV, 32), 0)
    total = jnp.zeros((DEV, SLOTS), F32)
    for values, shift in ((w, 0), (spot, CAP)):
        hot = jnp.where(rows == place + shift, 1.0, 0.0).astype(BF16)
        hi = values.astype(BF16)
        rest = values - hi.astype(F32)
        mid = rest.astype(BF16)
        low = (rest - mid.astype(F32)).astype(BF16)
        total = total + ((mm(hot, hi, NN) + mm(hot, mid, NN)) + mm(hot, low, NN))
    return total.reshape(16, 2 * CAP, SLOTS)


KR = 16
STEP = KR * SLOTS


def one_hots(land, zp, col):
    spot = land[:, CAP:].reshape(16 * CAP, SLOTS).astype(jnp.int32)
    weight = land[:, :CAP].reshape(16 * CAP, SLOTS)
    hi = weight.astype(BF16).astype(F32)
    lo = weight - hi
    z = spot & 511
    col[...] = spot >> 9
    rows = lax.broadcasted_iota(jnp.int32, (NG, SLOTS), 0)
    for r in range(16 * CAP):
        hit = rows == z[r : r + 1, :]
        at = slice(r * SLOTS, (r + 1) * SLOTS)
        zp[:NG, at] = jnp.where(hit, hi[r : r + 1, :], 0.0).astype(BF16)
        zp[NG:, at] = jnp.where(hit, lo[r : r + 1, :], 0.0).astype(BF16)


def paint_group(g, zp, col, spread, acc):
    rows = lax.broadcasted_iota(jnp.int32, (NG, SLOTS), 0) + g * NG
    for kk in range(16 * CAP // KR):
        for r in range(KR):
            hit = rows == col[kk * KR + r : kk * KR + r + 1, :]
            spread[:, r * SLOTS : (r + 1) * SLOTS] = jnp.where(hit, 1.0, 0.0).astype(BF16)
        both = mm(zp[:, kk * STEP : (kk + 1) * STEP], spread[...], NT)
        part = both[:NG] + both[NG:]
        if kk == 0:
            acc[...] = part
        else:
            acc[...] += part


ROOT = 0.8660254037844386


def three(a, b, c, inverse):
    tr, ti = b[0] + c[0], b[1] + c[1]
    dr, di = ROOT * (b[0] - c[0]), ROOT * (b[1] - c[1])
    er, ei = a[0] - 0.5 * tr, a[1] - 0.5 * ti
    one, two = (er + di, ei - dr), (er - di, ei + dr)
    return (a[0] + tr, a[1] + ti), *((two, one) if inverse else (one, two))


def nine(v, inverse):
    v = list(v)
    for x in range(3):
        v[3 * x : 3 * x + 3] = three(*v[3 * x : 3 * x + 3], inverse)
    for y in range(3):
        v[y], v[y + 3], v[y + 6] = three(v[y], v[y + 3], v[y + 6], inverse)
    return v


def turn(v, c, s):
    return v[0] * c - v[1] * s, v[0] * s + v[1] * c


RB = 16
def coords():
    px, py = lax.axis_index("px"), lax.axis_index("py")
    return px & 3, ((py >> 1) & 1) * 2 + (px >> 2), py >> 2, py & 1


def partner(t):
    x, y, z, core = coords()
    u = (t * 101) & 127
    sign = 1 - 2 * core
    x2 = (x + sign * ((u >> 1) & 3)) & 3
    y2 = (y + sign * ((u >> 3) & 3)) & 3
    z2 = (z + sign * ((u >> 5) & 3)) & 3
    return (y2 & 1) * 4 + x2, z2 * 4 + (y2 >> 1) * 2 + ((core + u) & 1)


def everyone(body):
    def step(t, carry):
        body(*partner(t))
        return carry

    lax.fori_loop(1, DEV, step, 0)


def fill_window(k, which, win):
    lane = lax.broadcasted_iota(jnp.int32, (RB, 128), 1)
    sub = lax.broadcasted_iota(jnp.int32, (RB, 128), 0)
    scale = jnp.where((k == 0) | (k == NG // 2), 1.0, 2.0) / float(NG) ** 3
    fz = signed(k)

    def step(i, carry):
        m, r = i // (DEV // RB), i % (DEV // RB)
        s = sub + r * RB
        bx = m // 3
        kx = (s >> 4) + 8 * bx + 24 * (lane >> 3)
        ky = (s & 15) + 16 * (m - 3 * bx) + 48 * (lane & 7)
        value = top_hat(signed(kx), signed(ky), fz) * scale
        win[which, pl.ds(pl.multiple_of(i * RB, RB), RB), :] = value
        return carry

    lax.fori_loop(0, CELLS // RB, step, 0)


def whole_body(
    ph, cell, count, owned, dens_hbm, table_hbm, tw_hbm, back_hbm, ah, al, bh, bl, ch, cl, dh, dl, out, ga_hbm, fa_hbm,
    dens, table, send, land, zp, col, spread, acc, f3, xg, xf, gs, fs,
    ys, rb, win, tw, back, ga, fa, stack, wide, tall, uh, ul, vh, vl, ss, rs, sg, rg, sf, rf, sy, ry, own, sl,
):
    px, py = lax.axis_index("px"), lax.axis_index("py")
    me = px * 16 + py
    loads = [
        pltpu.make_async_copy(a, b, sl.at[i])
        for i, (a, b) in enumerate(((dens_hbm, dens), (table_hbm, table), (tw_hbm, tw), (back_hbm, back)))
    ]
    for c in loads:
        c.start()
    barrier = pltpu.get_barrier_semaphore()
    everyone(lambda a, b: pl.semaphore_signal(barrier, inc=1, device_id=(a, b), device_id_type=MESH))
    send[...] = pack(ph[...], cell[...], count[...], owned[...])
    mine = pltpu.make_async_copy(send.at[py], land.at[py], own)
    mine.start()
    mine.wait()
    loads[0].wait()
    for m in range(9):
        xh, lh = m // 3, m % 3
        rows = [dens[(16 * xh + xl) * 24 + 8 * lh : (16 * xh + xl) * 24 + 8 * lh + 8, :] for xl in range(16)]
        hi, lo = cut(jnp.concatenate(rows, axis=0))
        at = slice(m * 128, (m + 1) * 128)
        stack[at, :NG] = hi
        stack[at, NG : 2 * NG] = lo
        stack[at, 2 * NG :] = hi
    pl.semaphore_wait(barrier, DEV - 1)
    for t in range(1, 16):
        to = (py + t) & 15
        pltpu.make_async_remote_copy(
            src_ref=send.at[to],
            dst_ref=land.at[py],
            send_sem=ss,
            recv_sem=rs,
            device_id=(px, to),
            device_id_type=MESH,
        ).start()
    loads[1].wait()
    res = mm(table[...], stack[...], NT)
    for c in range(3):
        xg[:, 0, c * CELLS : (c + 1) * CELLS] = res[c * DEV : (c + 1) * DEV]
    mine = pltpu.make_async_copy(xg.at[me], gs.at[me], own)
    mine.start()
    mine.wait()
    everyone(
        lambda a, b: pltpu.make_async_remote_copy(
            src_ref=xg.at[a * 16 + b],
            dst_ref=gs.at[me],
            send_sem=sg,
            recv_sem=rg,
            device_id=(a, b),
            device_id_type=MESH,
        ).start()
    )
    part = land.at[pl.ds(0, 15)]
    pltpu.make_async_copy(part, part, rs).wait()
    one_hots(land, zp, col)

    def one_group(g, carry):
        paint_group(g, zp, col, spread, acc)
        hi, lo = cut(acc[...])
        f3[:NG, :] = hi
        f3[NG : 2 * NG, :] = lo
        f3[2 * NG :, :] = hi
        res = mm(table[...], f3[...], NN)
        for c, first in enumerate((2 * DEV, 0, DEV)):
            xf[g, :, 0, c * NG : (c + 1) * NG] = res[first : first + DEV]
        mine = pltpu.make_async_copy(xf.at[g, me], fs.at[g, me], own)
        mine.start()
        mine.wait()
        everyone(
            lambda a, b: pltpu.make_async_remote_copy(
                src_ref=xf.at[g, a * 16 + b],
                dst_ref=fs.at[g, me],
                send_sem=sf.at[g],
                recv_sem=rf.at[g],
                device_id=(a, b),
                device_id_type=MESH,
            ).start()
        )
        return carry

    lax.fori_loop(0, 3, one_group, 0)
    fill_window(me + 1, 0, win)
    for c in loads[2:]:
        c.wait()
    part = gs.at[pl.ds(0, DEV - 1)]
    pltpu.make_async_copy(part, part, rg).wait()

    def one_plane(p, carry):
        @pl.when(p == 0)
        def _():
            for c in range(2):
                wide[c * DEV : (c + 1) * DEV, :] = gs[:, 0, c * CELLS : (c + 1) * CELLS]

        @pl.when(p == 1)
        def _():
            for g in range(3):
                part = fs.at[g, pl.ds(0, DEV - 1)]
                pltpu.make_async_copy(part, part, rf.at[g]).wait()
            wide[:DEV, :] = gs[:, 0, 2 * CELLS :]
            for g in range(3):
                wide[DEV:, g * NG : (g + 1) * NG] = fs[g, :, 0, :NG]

        @pl.when(p == 2)
        def _():
            for c in range(2):
                for g in range(3):
                    wide[c * DEV : (c + 1) * DEV, g * NG : (g + 1) * NG] = fs[g, :, 0, (c + 1) * NG : (c + 2) * NG]

        hi, lo = cut(wide[...])
        wide[...] = mm3(ah[...], al[...], hi, lo)

        def forward(i, inner):
            r = pl.multiple_of(i * RB, RB)
            v = []
            for m in range(9):
                cols = slice(m * 128, (m + 1) * 128)
                t = pl.ds(m * 128 + r, RB)
                u = (wide[pl.ds(r, RB), cols], wide[pl.ds(DEV + r, RB), cols])
                v.append(turn(u, tw[0, t, :], tw[1, t, :]))
            for m, u in enumerate(nine(v, False)):
                t = pl.ds(m * 128 + r, RB)
                for c, part in enumerate(turn(u, tw[2, t, :], tw[3, t, :])):
                    hi, lo = cut(part)
                    uh[t, c * 128 : (c + 1) * 128] = hi
                    ul[t, c * 128 : (c + 1) * 128] = lo
            return inner

        lax.fori_loop(0, DEV // RB, forward, 0)
        mid = mm3(uh[...], ul[...], ch[...], cl[...])
        this = win[p & 1]
        for c in range(2):
            hi, lo = cut(mid[:, c * 128 : (c + 1) * 128] * this)
            uh[:, c * 128 : (c + 1) * 128] = hi
            ul[:, c * 128 : (c + 1) * 128] = lo
        tall[...] = mm3(uh[...], ul[...], dh[...], dl[...])

        def backward(i, inner):
            r = pl.multiple_of(i * RB, RB)
            v = []
            for m in range(9):
                t = pl.ds(m * 128 + r, RB)
                v.append(turn((tall[t, :128], tall[t, 128:]), tw[2, t, :], -tw[3, t, :]))
            for m, u in enumerate(nine(v, True)):
                t = pl.ds(m * 128 + r, RB)
                cols = slice(m * 128, (m + 1) * 128)
                for c, part in enumerate(turn(u, tw[0, t, :], -tw[1, t, :])):
                    hi, lo = cut(part)
                    vh[pl.ds(c * DEV + r, RB), cols] = hi
                    vl[pl.ds(c * DEV + r, RB), cols] = lo
            return inner

        lax.fori_loop(0, DEV // RB, backward, 0)
        back = mm3(bh[...], bl[...], vh[...], vl[...])
        for c in range(2):
            ys[p, :, 0, c * CELLS : (c + 1) * CELLS] = back[c * DEV : (c + 1) * DEV]
        def give(home, q):
            mine = pltpu.make_async_copy(ys.at[p, me], home.at[q, me], own)
            mine.start()
            mine.wait()
            everyone(
                lambda a, b: pltpu.make_async_remote_copy(
                    src_ref=ys.at[p, a * 16 + b],
                    dst_ref=home.at[q, me],
                    send_sem=sy.at[p],
                    recv_sem=ry.at[p],
                    device_id=(a, b),
                    device_id_type=MESH,
                ).start()
            )

        @pl.when(p < 2)
        def _():
            give(rb, jnp.minimum(p, 1))

        @pl.when(p == 2)
        def _():
            give(out, 0)

        @pl.when(p == 0)
        def _():
            second = jnp.where(me < 63, 129 + me, jnp.where(me < 126, 66 + me, (me - 126) * (NG // 2)))
            fill_window(second, 1, win)

        return carry

    lax.fori_loop(0, 3, one_plane, 0)
    for p in range(2):
        part = rb.at[p, pl.ds(0, DEV - 1)]
        pltpu.make_async_copy(part, part, ry.at[p]).wait()
    for i, (p, c) in enumerate(((0, 0), (0, 1), (1, 0), (1, 1))):
        hi, lo = cut(rb[p, :, 0, c * CELLS : (c + 1) * CELLS])
        at = (i % 3) * DEV
        if i < 3:
            stack[at : at + DEV, :] = hi
            stack[NG + at : NG + at + DEV, :] = lo
            stack[2 * NG + at : 2 * NG + at + DEV, :] = hi
        if i == 2:
            ga[...] = mm(back[...], stack[...], NN)
        if i == 3:
            cols = slice(2 * DEV, 3 * DEV)
            fa[...] = (mm(back[:, cols], hi, NN) + mm(back[:, cols], lo, NN)) + mm(back[:, 2 * NG + 2 * DEV :], hi, NN)
    stores = [pltpu.make_async_copy(ga, ga_hbm, sl.at[0]), pltpu.make_async_copy(fa, fa_hbm, sl.at[1])]
    for c in stores:
        c.start()
    part = send.at[pl.ds(0, 15)]
    pltpu.make_async_copy(part, part, ss).wait()
    part = xg.at[pl.ds(0, DEV - 1)]
    pltpu.make_async_copy(part, part, sg).wait()
    for g in range(3):
        part = xf.at[g, pl.ds(0, DEV - 1)]
        pltpu.make_async_copy(part, part, sf.at[g]).wait()
    for p in range(3):
        part = ys.at[p, pl.ds(0, DEV - 1)]
        pltpu.make_async_copy(part, part, sy.at[p]).wait()
    for c in stores:
        c.wait()
    part = out.at[0, pl.ds(0, DEV - 1)]
    pltpu.make_async_copy(part, part, ry.at[2]).wait()


def last_body(r_hbm, ga_hbm, fa_hbm, table_hbm, out_hbm, r, ga, fa, table, stack, out, sem, done):
    loads = [
        pltpu.make_async_copy(a, b, sem.at[i])
        for i, (a, b) in enumerate(((r_hbm.at[0], r), (table_hbm, table), (fa_hbm, fa), (ga_hbm, ga)))
    ]
    for c in loads:
        c.start()
    loads[0].wait()
    for c in range(2):
        hi, lo = cut(r[:, 0, c * CELLS : (c + 1) * CELLS])
        at = c * DEV
        stack[at : at + DEV, :] = hi
        stack[2 * DEV + at : 2 * DEV + at + DEV, :] = lo
        stack[4 * DEV + at : 4 * DEV + at + DEV, :] = hi
    loads[1].wait()
    left = jnp.concatenate([table[:, i * NG : i * NG + 2 * DEV] for i in range(3)], axis=1)
    stores = []
    for xh in range(3):
        whole = slice(xh * NG, (xh + 1) * NG)
        f = mm(left, stack[:, whole], NN)
        if xh == 0:
            for c in loads[2:]:
                c.wait()
        f = fa[:, whole] + f
        frac = jnp.clip(f / jnp.maximum(ga[:, whole], 0.5), 0.0, 1.0)
        for lh in range(3):
            turned = frac[:, lh * 128 : (lh + 1) * 128].T
            for xl in range(16):
                at = (16 * xh + xl) * 24 + 8 * lh
                out[at : at + 8, :] = turned[xl * 8 : xl * 8 + 8, :]
        c = pltpu.make_async_copy(out.at[pl.ds(xh * NG, NG)], out_hbm.at[pl.ds(xh * NG, NG)], done.at[xh])
        c.start()
        stores.append(c)
    for c in stores:
        c.wait()


def sds(*shape, dtype=F32):
    return jax.ShapeDtypeStruct(shape, dtype)


def whole(halos, density, ahead, tw, back, mats):
    dma = pltpu.SemaphoreType.DMA
    plane = (DEV, 1, PLANE)
    anywhere, here = pl.BlockSpec(memory_space=pl.ANY), pl.BlockSpec(memory_space=VMEM)
    return pl.pallas_call(
        whole_body,
        out_shape=(sds(1, *plane), sds(NG, CELLS), sds(NG, CELLS)),
        in_specs=[here] * 4 + [anywhere] * 4 + [here] * 8,
        out_specs=(anywhere,) * 3,
        scratch_shapes=[
            VMEM((CELLS, NG), F32),
            VMEM((NG, 3 * NG), BF16),
            VMEM((16, 2 * CAP, SLOTS), F32),
            VMEM((16, 2 * CAP, SLOTS), F32),
            VMEM((2 * NG, 16 * CAP * SLOTS), BF16),
            VMEM((16 * CAP, SLOTS), jnp.int32),
            VMEM((NG, STEP), BF16),
            VMEM((NG, NG), F32),
            VMEM((3 * NG, NG), BF16),
            VMEM((DEV, 1, HALF), F32),
            VMEM((3, DEV, 1, CELLS), F32),
            VMEM((DEV, 1, HALF), F32),
            VMEM((3, DEV, 1, CELLS), F32),
            VMEM((3, *plane), F32),
            VMEM((2, *plane), F32),
            VMEM((2, CELLS, 128), F32),
            VMEM((4, CELLS, 128), F32),
            VMEM((NG, 3 * NG), BF16),
            VMEM((NG, CELLS), F32),
            VMEM((NG, CELLS), F32),
            VMEM((3 * NG, CELLS), BF16),
            VMEM((256, CELLS), F32),
            VMEM((CELLS, 256), F32),
            VMEM((CELLS, 256), BF16),
            VMEM((CELLS, 256), BF16),
            VMEM((256, CELLS), BF16),
            VMEM((256, CELLS), BF16),
            dma,
            dma,
            dma,
            dma,
            dma((3,)),
            dma((3,)),
            dma((3,)),
            dma((3,)),
            dma,
            dma((4,)),
        ],
        compiler_params=pltpu.CompilerParams(vmem_limit_bytes=63 << 20, collective_id=1, has_side_effects=True),
        cost_estimate=pl.CostEstimate(flops=36 << 30, bytes_accessed=8 << 20, transcendentals=0),
        name="whole",
    )(*halos, density, ahead, tw, back, *mats)


def on_device(photons, halo_cells, halo_counts, owners, density):
    table = z_table()
    ahead, back = stacked(table, 1), stacked(table.T, 1)
    mats = []
    for m in (row_matrix(1), row_matrix(-1), lane_matrix(1), lane_matrix(-1)):
        mats += [jnp.asarray(t) for t in cut_np(m)]

    dma = pltpu.SemaphoreType.DMA
    halos = (photons, halo_cells, halo_counts.reshape(1, 32), owners.reshape(1, 32))
    r, ga, fa = whole(halos, density.reshape(CELLS, NG), ahead, jnp.asarray(twiddles()), back, mats)
    anywhere = pl.BlockSpec(memory_space=pl.ANY)
    out = pl.pallas_call(
        last_body,
        out_shape=sds(CELLS, NG),
        in_specs=[anywhere] * 4,
        out_specs=anywhere,
        scratch_shapes=[VMEM((DEV, 1, PLANE), F32), VMEM((NG, CELLS), F32), VMEM((NG, CELLS), F32)]
        + [VMEM((NG, 3 * NG), BF16), VMEM((6 * DEV, CELLS), BF16), VMEM((CELLS, NG), F32), dma((4,)), dma((3,))],
        compiler_params=pltpu.CompilerParams(vmem_limit_bytes=LIMIT),
        cost_estimate=pl.CostEstimate(flops=1 << 30, bytes_accessed=6 << 20, transcendentals=0),
        name="last",
    )(r, ga, fa, back)
    return out.reshape(48, 24, NG)


def solution(mesh):
    placed = (
        P(("px", "py"), None),
        P(("px", "py"), None),
        P(("px", "py")),
        P(("px", "py"), None),
        P("px", "py", None),
    )
    return jax.shard_map(
        on_device, mesh=mesh, in_specs=placed, out_specs=P("px", "py", None), check_vma=False
    )
```

```python
import functools

import jax
import jax.numpy as jnp
import numpy as np
from jax import lax
from jax.experimental import pallas as pl
from jax.experimental.pallas import tpu as pltpu
from jax.sharding import PartitionSpec as P

NG = 384
SLOTS = 128
CAP = 4
RADIUS = 20
DEV = 128
CELLS = 1152
PLANE = 2 * CELLS
HALF = 3 * CELLS
LIMIT = 60 * 1024 * 1024
F32 = jnp.float32
BF16 = jnp.bfloat16
VMEM = pltpu.VMEM
MESH = pl.DeviceIdType.MESH


def cut(v):
    hi = v.astype(BF16)
    return hi, (v - hi.astype(F32)).astype(BF16)


def cut_np(v):
    v = np.asarray(v, np.float32)
    hi = v.astype(jnp.bfloat16)
    lo = (v - hi.astype(np.float32)).astype(jnp.bfloat16)
    return hi, lo


NN = (((1,), (0,)), ((), ()))
NT = (((1,), (1,)), ((), ()))


def mm(a, b, dims):
    return lax.dot_general(a, b, dims, preferred_element_type=F32)


def mm3(ah, al, bh, bl, dims=NN):
    return mm(ah, bh, dims) + (mm(ah, bl, dims) + mm(al, bh, dims))


def z_table():
    k = np.arange(1, NG // 2)[:, None] * np.arange(NG)[None]
    angle = 2 * np.pi * (k % NG) / NG
    c, s = np.cos(angle), np.sin(angle)
    ends = np.stack([np.ones(NG), 1.0 - 2.0 * (np.arange(NG) % 2)])
    return np.concatenate([c[:DEV], s[:DEV], c[DEV:], s[DEV:], ends])


def stacked(v, axis):
    hi, lo = cut_np(v)
    return jnp.asarray(np.concatenate([hi, hi, lo], axis=axis))


def mix(left, right):
    i = np.arange(left * right)
    a, b = i // right, i % right
    ph = -2j * np.pi * (np.outer(a, a) / left + np.outer(b, b) / right)
    return np.exp(ph)


def row_matrix(sign):
    m = mix(8, 16)
    re, im = m.real, sign * m.imag
    return np.block([[re, -im], [im, re]])


def lane_matrix(sign):
    m = mix(16, 8)
    re, im = m.real, sign * m.imag
    return np.block([[re, im], [-im, re]])


def twiddles():
    row, lane = np.arange(CELLS)[:, None], np.arange(128)[None]
    m, s = row // 128, row % 128
    ax, ay, bx, by, cx, cy = s // 16, s % 16, m // 3, m % 3, lane // 8, lane % 8
    one = (ax * bx * 16 + ay * by * 8 + 0 * lane) * (2 * np.pi / NG)
    two = (cx * (ax + 8 * bx) + cy * (ay + 16 * by)) * (2 * np.pi / NG)
    return np.stack([np.cos(one), -np.sin(one), np.cos(two), -np.sin(two)]).astype(np.float32)


def signed(k):
    return jnp.where(k < NG // 2, k, k - NG).astype(F32)


def top_hat(freq_x, freq_y, freq_z):
    radial = jnp.sqrt(freq_x * freq_x + freq_y * freq_y + freq_z * freq_z) * (2.0 * jnp.pi * RADIUS / NG)
    safe = jnp.where(radial > 0, radial, 1.0)
    value = 3.0 * (jnp.sin(safe) - safe * jnp.cos(safe)) / (safe * safe * safe)
    return jnp.where(radial > 0, value, 1.0)


def pack(photons, cells, counts, owned):
    lane = lax.broadcasted_iota(jnp.int32, (32, SLOTS), 1)
    first = lax.broadcasted_iota(jnp.int32, (32, 32), 0)
    second = lax.broadcasted_iota(jnp.int32, (32, 32), 1)

    def column(row):
        spread = jnp.where(first == second, row.astype(F32), 0.0)
        return jnp.sum(spread, axis=1, keepdims=True).astype(jnp.int32)

    live = lane < column(counts)
    w = jnp.where(live, photons, 0.0)
    cell = jnp.where(live, cells, 0)
    column_of = cell // NG
    gz = cell - column_of * NG
    gx = column_of // 24
    gy = column_of - gx * 24
    place_in = ((gx >> 4) * 3 + (gy >> 3)) * 128 + (gx & 15) * 8 + (gy & 7)
    spot = (place_in * 512 + gz).astype(F32)
    same = (column(owned) == owned) & (first < second)
    rank = jnp.sum(jnp.where(same, 1.0, 0.0), axis=0, keepdims=True).astype(jnp.int32)
    place = owned * (2 * CAP) + rank
    rows = lax.broadcasted_iota(jnp.int32, (DEV, 32), 0)
    total = jnp.zeros((DEV, SLOTS), F32)
    for values, shift in ((w, 0), (spot, CAP)):
        hot = jnp.where(rows == place + shift, 1.0, 0.0).astype(BF16)
        hi = values.astype(BF16)
        rest = values - hi.astype(F32)
        mid = rest.astype(BF16)
        low = (rest - mid.astype(F32)).astype(BF16)
        total = total + ((mm(hot, hi, NN) + mm(hot, mid, NN)) + mm(hot, low, NN))
    return total.reshape(16, 2 * CAP, SLOTS)


KR = 16
STEP = KR * SLOTS


def one_hots(land, zp, col):
    spot = land[:, CAP:].reshape(16 * CAP, SLOTS).astype(jnp.int32)
    weight = land[:, :CAP].reshape(16 * CAP, SLOTS)
    hi = weight.astype(BF16).astype(F32)
    lo = weight - hi
    z = spot & 511
    col[...] = spot >> 9
    rows = lax.broadcasted_iota(jnp.int32, (NG, SLOTS), 0)
    for r in range(16 * CAP):
        hit = rows == z[r : r + 1, :]
        at = slice(r * SLOTS, (r + 1) * SLOTS)
        zp[:NG, at] = jnp.where(hit, hi[r : r + 1, :], 0.0).astype(BF16)
        zp[NG:, at] = jnp.where(hit, lo[r : r + 1, :], 0.0).astype(BF16)


def paint_group(g, zp, col, spread, acc):
    rows = lax.broadcasted_iota(jnp.int32, (NG, SLOTS), 0) + g * NG
    for kk in range(16 * CAP // KR):
        for r in range(KR):
            hit = rows == col[kk * KR + r : kk * KR + r + 1, :]
            spread[:, r * SLOTS : (r + 1) * SLOTS] = jnp.where(hit, 1.0, 0.0).astype(BF16)
        both = mm(zp[:, kk * STEP : (kk + 1) * STEP], spread[...], NT)
        part = both[:NG] + both[NG:]
        if kk == 0:
            acc[...] = part
        else:
            acc[...] += part


ROOT = 0.8660254037844386


def three(a, b, c, inverse):
    tr, ti = b[0] + c[0], b[1] + c[1]
    dr, di = ROOT * (b[0] - c[0]), ROOT * (b[1] - c[1])
    er, ei = a[0] - 0.5 * tr, a[1] - 0.5 * ti
    one, two = (er + di, ei - dr), (er - di, ei + dr)
    return (a[0] + tr, a[1] + ti), *((two, one) if inverse else (one, two))


def nine(v, inverse):
    v = list(v)
    for x in range(3):
        v[3 * x : 3 * x + 3] = three(*v[3 * x : 3 * x + 3], inverse)
    for y in range(3):
        v[y], v[y + 3], v[y + 6] = three(v[y], v[y + 3], v[y + 6], inverse)
    return v


def turn(v, c, s):
    return v[0] * c - v[1] * s, v[0] * s + v[1] * c


RB = 16
BATCH = 14


def everyone(body):
    me = lax.axis_index("px") * 16 + lax.axis_index("py")

    def one(t):
        other = me ^ ((t * 101) & (DEV - 1))
        body(other, (other >> 4, other & 15))

    def step(i, carry):
        for u in range(BATCH):
            one(1 + i * BATCH + u)
        return carry

    lax.fori_loop(0, (DEV - 2) // BATCH, step, 0)
    one(DEV - 1)


def fill_window(k, which, win):
    lane = lax.broadcasted_iota(jnp.int32, (RB, 128), 1)
    sub = lax.broadcasted_iota(jnp.int32, (RB, 128), 0)
    scale = jnp.where((k == 0) | (k == NG // 2), 1.0, 2.0) / float(NG) ** 3
    fz = signed(k)

    def step(i, carry):
        m, r = i // (DEV // RB), i % (DEV // RB)
        s = sub + r * RB
        bx = m // 3
        kx = (s >> 4) + 8 * bx + 24 * (lane >> 3)
        ky = (s & 15) + 16 * (m - 3 * bx) + 48 * (lane & 7)
        value = top_hat(signed(kx), signed(ky), fz) * scale
        win[which, pl.ds(pl.multiple_of(i * RB, RB), RB), :] = value
        return carry

    lax.fori_loop(0, CELLS // RB, step, 0)


def whole_body(
    ph, cell, count, owned, dens_hbm, table_hbm, tw_hbm, back_hbm, ah, al, bh, bl, ch, cl, dh, dl, result,
    dens, table, send, land, zp, col, spread, acc, f3, xg, xf, gs, fs, out,
    ys, rb, win, tw, back, ga, fa, stack, wide, tall, uh, ul, vh, vl, ss, rs, sg, rg, sf, rf, sy, ry, own, sl,
):
    px, py = lax.axis_index("px"), lax.axis_index("py")
    me = px * 16 + py
    loads = [
        pltpu.make_async_copy(a, b, sl.at[i])
        for i, (a, b) in enumerate(((dens_hbm, dens), (table_hbm, table), (tw_hbm, tw), (back_hbm, back)))
    ]
    for c in loads:
        c.start()
    barrier = pltpu.get_barrier_semaphore()
    everyone(lambda i, to: pl.semaphore_signal(barrier, inc=1, device_id=to, device_id_type=MESH))
    send[...] = pack(ph[...], cell[...], count[...], owned[...])
    halo_own = pltpu.make_async_copy(send.at[py], land.at[py], own.at[0])
    halo_own.start()
    loads[0].wait()
    for m in range(9):
        xh, lh = m // 3, m % 3
        rows = [dens[(16 * xh + xl) * 24 + 8 * lh : (16 * xh + xl) * 24 + 8 * lh + 8, :] for xl in range(16)]
        hi, lo = cut(jnp.concatenate(rows, axis=0))
        at = slice(m * 128, (m + 1) * 128)
        stack[at, :NG] = hi
        stack[at, NG : 2 * NG] = lo
        stack[at, 2 * NG :] = hi
    pl.semaphore_wait(barrier, DEV - 1)
    for t in range(1, 16):
        to = (py + t) & 15
        pltpu.make_async_remote_copy(
            src_ref=send.at[to],
            dst_ref=land.at[py],
            send_sem=ss,
            recv_sem=rs,
            device_id=(px, to),
            device_id_type=MESH,
        ).start()
    loads[1].wait()
    res = mm(table[...], stack[...], NT)
    for c in range(3):
        xg[:, 0, c * CELLS : (c + 1) * CELLS] = res[c * DEV : (c + 1) * DEV]
    density_own = pltpu.make_async_copy(xg.at[me], gs.at[me], own.at[1])
    density_own.start()
    everyone(
        lambda i, to: pltpu.make_async_remote_copy(
            src_ref=xg.at[i],
            dst_ref=gs.at[me],
            send_sem=sg,
            recv_sem=rg,
            device_id=to,
            device_id_type=MESH,
        ).start()
    )
    fill_window(me + 1, 0, win)
    halo_own.wait()
    part = land.at[pl.ds(0, 15)]
    pltpu.make_async_copy(part, part, rs).wait()
    one_hots(land, zp, col)

    def one_group(g, carry):
        paint_group(g, zp, col, spread, acc)
        hi, lo = cut(acc[...])
        f3[:NG, :] = hi
        f3[NG : 2 * NG, :] = lo
        f3[2 * NG :, :] = hi
        res = mm(table[...], f3[...], NN)
        for c, first in enumerate((2 * DEV, 0, DEV)):
            xf[g, :, 0, c * NG : (c + 1) * NG] = res[first : first + DEV]
        pltpu.make_async_copy(xf.at[g, me], fs.at[g, me], own.at[2 + g]).start()
        everyone(
            lambda i, to: pltpu.make_async_remote_copy(
                src_ref=xf.at[g, i],
                dst_ref=fs.at[g, me],
                send_sem=sf.at[g],
                recv_sem=rf.at[g],
                device_id=to,
                device_id_type=MESH,
            ).start()
        )
        return carry

    lax.fori_loop(0, 3, one_group, 0)
    density_own.wait()
    for c in loads[2:]:
        c.wait()
    part = gs.at[pl.ds(0, DEV - 1)]
    pltpu.make_async_copy(part, part, rg).wait()

    def one_plane(p, carry):
        @pl.when(p == 0)
        def _():
            for c in range(2):
                wide[c * DEV : (c + 1) * DEV, :] = gs[:, 0, c * CELLS : (c + 1) * CELLS]

        @pl.when(p == 1)
        def _():
            for g in range(3):
                pltpu.make_async_copy(xf.at[g, me], fs.at[g, me], own.at[2 + g]).wait()
                part = fs.at[g, pl.ds(0, DEV - 1)]
                pltpu.make_async_copy(part, part, rf.at[g]).wait()
            wide[:DEV, :] = gs[:, 0, 2 * CELLS :]
            for g in range(3):
                wide[DEV:, g * NG : (g + 1) * NG] = fs[g, :, 0, :NG]

        @pl.when(p == 2)
        def _():
            for c in range(2):
                for g in range(3):
                    wide[c * DEV : (c + 1) * DEV, g * NG : (g + 1) * NG] = fs[g, :, 0, (c + 1) * NG : (c + 2) * NG]

        hi, lo = cut(wide[...])
        wide[...] = mm3(ah[...], al[...], hi, lo)

        def forward(i, inner):
            r = pl.multiple_of(i * RB, RB)
            v = []
            for m in range(9):
                cols = slice(m * 128, (m + 1) * 128)
                t = pl.ds(m * 128 + r, RB)
                u = (wide[pl.ds(r, RB), cols], wide[pl.ds(DEV + r, RB), cols])
                v.append(turn(u, tw[0, t, :], tw[1, t, :]))
            for m, u in enumerate(nine(v, False)):
                t = pl.ds(m * 128 + r, RB)
                for c, part in enumerate(turn(u, tw[2, t, :], tw[3, t, :])):
                    hi, lo = cut(part)
                    uh[t, c * 128 : (c + 1) * 128] = hi
                    ul[t, c * 128 : (c + 1) * 128] = lo
            return inner

        lax.fori_loop(0, DEV // RB, forward, 0)
        mid = mm3(uh[...], ul[...], ch[...], cl[...])
        this = win[p & 1]
        for c in range(2):
            hi, lo = cut(mid[:, c * 128 : (c + 1) * 128] * this)
            uh[:, c * 128 : (c + 1) * 128] = hi
            ul[:, c * 128 : (c + 1) * 128] = lo
        tall[...] = mm3(uh[...], ul[...], dh[...], dl[...])

        def backward(i, inner):
            r = pl.multiple_of(i * RB, RB)
            v = []
            for m in range(9):
                t = pl.ds(m * 128 + r, RB)
                v.append(turn((tall[t, :128], tall[t, 128:]), tw[2, t, :], -tw[3, t, :]))
            for m, u in enumerate(nine(v, True)):
                t = pl.ds(m * 128 + r, RB)
                cols = slice(m * 128, (m + 1) * 128)
                for c, part in enumerate(turn(u, tw[0, t, :], -tw[1, t, :])):
                    hi, lo = cut(part)
                    vh[pl.ds(c * DEV + r, RB), cols] = hi
                    vl[pl.ds(c * DEV + r, RB), cols] = lo
            return inner

        lax.fori_loop(0, DEV // RB, backward, 0)
        back = mm3(bh[...], bl[...], vh[...], vl[...])
        for c in range(2):
            ys[p, :, 0, c * CELLS : (c + 1) * CELLS] = back[c * DEV : (c + 1) * DEV]
        pltpu.make_async_copy(ys.at[p, me], rb.at[p, me], own.at[5 + p]).start()
        everyone(
            lambda i, to: pltpu.make_async_remote_copy(
                src_ref=ys.at[p, i],
                dst_ref=rb.at[p, me],
                send_sem=sy.at[p],
                recv_sem=ry.at[p],
                device_id=to,
                device_id_type=MESH,
            ).start()
        )

        @pl.when(p == 0)
        def _():
            second = jnp.where(me < 63, 129 + me, jnp.where(me < 126, 66 + me, (me - 126) * (NG // 2)))
            fill_window(second, 1, win)

        return carry

    lax.fori_loop(0, 3, one_plane, 0)
    for p in range(2):
        pltpu.make_async_copy(ys.at[p, me], rb.at[p, me], own.at[5 + p]).wait()
        part = rb.at[p, pl.ds(0, DEV - 1)]
        pltpu.make_async_copy(part, part, ry.at[p]).wait()
    for i, (p, c) in enumerate(((0, 0), (0, 1), (1, 0), (1, 1))):
        spot = (i % 2) * DEV
        wide[spot : spot + DEV, :] = rb[p, :, 0, c * CELLS : (c + 1) * CELLS]
        hi, lo = cut(wide[spot : spot + DEV, :])
        at = (i % 3) * DEV
        if i < 3:
            stack[at : at + DEV, :] = hi
            stack[NG + at : NG + at + DEV, :] = lo
            stack[2 * NG + at : 2 * NG + at + DEV, :] = hi
        if i == 2:
            ga[...] = mm(back[...], stack[...], NN)
        if i == 3:
            cols = slice(2 * DEV, 3 * DEV)
            fa[...] = (mm(back[:, cols], hi, NN) + mm(back[:, cols], lo, NN)) + mm(back[:, 2 * NG + 2 * DEV :], hi, NN)
    part = send.at[pl.ds(0, 15)]
    pltpu.make_async_copy(part, part, ss).wait()
    part = xg.at[pl.ds(0, DEV - 1)]
    pltpu.make_async_copy(part, part, sg).wait()
    for g in range(3):
        part = xf.at[g, pl.ds(0, DEV - 1)]
        pltpu.make_async_copy(part, part, sf.at[g]).wait()
    for p in range(3):
        part = ys.at[p, pl.ds(0, DEV - 1)]
        pltpu.make_async_copy(part, part, sy.at[p]).wait()
    pltpu.make_async_copy(ys.at[2, me], rb.at[2, me], own.at[7]).wait()
    part = rb.at[2, pl.ds(0, DEV - 1)]
    pltpu.make_async_copy(part, part, ry.at[2]).wait()
    for c in range(2):
        at = c * DEV
        wide[at : at + DEV, :] = rb[2, :, 0, c * CELLS : (c + 1) * CELLS]
        hi, lo = cut(wide[at : at + DEV, :])
        stack[at : at + DEV, :] = hi
        stack[2 * DEV + at : 2 * DEV + at + DEV, :] = lo
        stack[4 * DEV + at : 4 * DEV + at + DEV, :] = hi
    left = jnp.concatenate([back[:, i * NG : i * NG + 2 * DEV] for i in range(3)], axis=1)
    stores = []
    for xh in range(3):
        cols = slice(xh * NG, (xh + 1) * NG)
        f = fa[:, cols] + mm(left, stack[: 6 * DEV, cols], NN)
        frac = jnp.clip(f / jnp.maximum(ga[:, cols], 0.5), 0.0, 1.0)
        for lh in range(3):
            turned = frac[:, lh * 128 : (lh + 1) * 128].T
            for xl in range(16):
                at = (16 * xh + xl) * 24 + 8 * lh
                out[at : at + 8, :] = turned[xl * 8 : xl * 8 + 8, :]
        c = pltpu.make_async_copy(out.at[pl.ds(xh * NG, NG)], result.at[pl.ds(xh * NG, NG)], sl.at[xh])
        c.start()
        stores.append(c)
    for c in stores:
        c.wait()


def sds(*shape, dtype=F32):
    return jax.ShapeDtypeStruct(shape, dtype)


def whole(halos, density, ahead, tw, back, mats):
    dma = pltpu.SemaphoreType.DMA
    plane = (DEV, 1, PLANE)
    anywhere, here = pl.BlockSpec(memory_space=pl.ANY), pl.BlockSpec(memory_space=VMEM)
    return pl.pallas_call(
        whole_body,
        out_shape=sds(CELLS, NG),
        in_specs=[here] * 4 + [anywhere] * 4 + [here] * 8,
        out_specs=anywhere,
        scratch_shapes=[
            VMEM((CELLS, NG), F32),
            VMEM((NG, 3 * NG), BF16),
            VMEM((16, 2 * CAP, SLOTS), F32),
            VMEM((16, 2 * CAP, SLOTS), F32),
            VMEM((2 * NG, 16 * CAP * SLOTS), BF16),
            VMEM((16 * CAP, SLOTS), jnp.int32),
            VMEM((NG, STEP), BF16),
            VMEM((NG, NG), F32),
            VMEM((3 * NG, NG), BF16),
            VMEM((DEV, 1, HALF), F32),
            VMEM((3, DEV, 1, CELLS), F32),
            VMEM((DEV, 1, HALF), F32),
            VMEM((3, DEV, 1, CELLS), F32),
            VMEM((CELLS, NG), F32),
            VMEM((3, *plane), F32),
            VMEM((3, *plane), F32),
            VMEM((2, CELLS, 128), F32),
            VMEM((4, CELLS, 128), F32),
            VMEM((NG, 3 * NG), BF16),
            VMEM((NG, CELLS), F32),
            VMEM((NG, CELLS), F32),
            VMEM((3 * NG, CELLS), BF16),
            VMEM((256, CELLS), F32),
            VMEM((CELLS, 256), F32),
            VMEM((CELLS, 256), BF16),
            VMEM((CELLS, 256), BF16),
            VMEM((256, CELLS), BF16),
            VMEM((256, CELLS), BF16),
            dma,
            dma,
            dma,
            dma,
            dma((3,)),
            dma((3,)),
            dma((3,)),
            dma((3,)),
            dma((8,)),
            dma((4,)),
        ],
        compiler_params=pltpu.CompilerParams(vmem_limit_bytes=63 << 20, collective_id=1, has_side_effects=True),
        cost_estimate=pl.CostEstimate(flops=36 << 30, bytes_accessed=8 << 20, transcendentals=0),
        name="whole",
    )(*halos, density, ahead, tw, back, *mats)


def on_device(photons, halo_cells, halo_counts, owners, density):
    table = z_table()
    ahead, back = stacked(table, 1), stacked(table.T, 1)
    mats = []
    for m in (row_matrix(1), row_matrix(-1), lane_matrix(1), lane_matrix(-1)):
        mats += [jnp.asarray(t) for t in cut_np(m)]

    halos = (photons, halo_cells, halo_counts.reshape(1, 32), owners.reshape(1, 32))
    out = whole(halos, density.reshape(CELLS, NG), ahead, jnp.asarray(twiddles()), back, mats)
    return out.reshape(48, 24, NG)


def solution(mesh):
    placed = (
        P(("px", "py"), None),
        P(("px", "py"), None),
        P(("px", "py")),
        P(("px", "py"), None),
        P("px", "py", None),
    )
    return jax.shard_map(
        on_device, mesh=mesh, in_specs=placed, out_specs=P("px", "py", None), check_vma=False
    )
```

```python
import functools

import jax
import jax.numpy as jnp
import numpy as np
from jax import lax
from jax.experimental import pallas as pl
from jax.experimental.pallas import tpu as pltpu
from jax.sharding import PartitionSpec as P

NG = 384
SLOTS = 128
CAP = 4
RADIUS = 20
DEV = 128
CELLS = 1152
PLANE = 2 * CELLS
HALF = 3 * CELLS
LIMIT = 60 * 1024 * 1024
F32 = jnp.float32
BF16 = jnp.bfloat16
VMEM = pltpu.VMEM
MESH = pl.DeviceIdType.MESH


def cut(v):
    hi = v.astype(BF16)
    return hi, (v - hi.astype(F32)).astype(BF16)


def cut_np(v):
    v = np.asarray(v, np.float32)
    hi = v.astype(jnp.bfloat16)
    lo = (v - hi.astype(np.float32)).astype(jnp.bfloat16)
    return hi, lo


NN = (((1,), (0,)), ((), ()))
NT = (((1,), (1,)), ((), ()))


def mm(a, b, dims):
    return lax.dot_general(a, b, dims, preferred_element_type=F32)


def mm3(ah, al, bh, bl, dims=NN):
    return mm(ah, bh, dims) + (mm(ah, bl, dims) + mm(al, bh, dims))


def z_table():
    k = np.arange(1, NG // 2)[:, None] * np.arange(NG)[None]
    angle = 2 * np.pi * (k % NG) / NG
    c, s = np.cos(angle), np.sin(angle)
    ends = np.stack([np.ones(NG), 1.0 - 2.0 * (np.arange(NG) % 2)])
    return np.concatenate([c[:DEV], s[:DEV], c[DEV:], s[DEV:], ends])


def stacked(v, axis):
    hi, lo = cut_np(v)
    return jnp.asarray(np.concatenate([hi, hi, lo], axis=axis))


def mix(left, right):
    i = np.arange(left * right)
    a, b = i // right, i % right
    ph = -2j * np.pi * (np.outer(a, a) / left + np.outer(b, b) / right)
    return np.exp(ph)


def row_matrix(sign):
    m = mix(8, 16)
    re, im = m.real, sign * m.imag
    return np.block([[re, -im], [im, re]])


def lane_matrix(sign):
    m = mix(16, 8)
    re, im = m.real, sign * m.imag
    return np.block([[re, im], [-im, re]])


def twiddles():
    row, lane = np.arange(CELLS)[:, None], np.arange(128)[None]
    m, s = row // 128, row % 128
    ax, ay, bx, by, cx, cy = s // 16, s % 16, m // 3, m % 3, lane // 8, lane % 8
    one = (ax * bx * 16 + ay * by * 8 + 0 * lane) * (2 * np.pi / NG)
    two = (cx * (ax + 8 * bx) + cy * (ay + 16 * by)) * (2 * np.pi / NG)
    return np.stack([np.cos(one), -np.sin(one), np.cos(two), -np.sin(two)]).astype(np.float32)


def signed(k):
    return jnp.where(k < NG // 2, k, k - NG).astype(F32)


def top_hat(freq_x, freq_y, freq_z):
    radial = jnp.sqrt(freq_x * freq_x + freq_y * freq_y + freq_z * freq_z) * (2.0 * jnp.pi * RADIUS / NG)
    safe = jnp.where(radial > 0, radial, 1.0)
    value = 3.0 * (jnp.sin(safe) - safe * jnp.cos(safe)) / (safe * safe * safe)
    return jnp.where(radial > 0, value, 1.0)


def pack(photons, cells, counts, owned):
    lane = lax.broadcasted_iota(jnp.int32, (32, SLOTS), 1)
    first = lax.broadcasted_iota(jnp.int32, (32, 32), 0)
    second = lax.broadcasted_iota(jnp.int32, (32, 32), 1)

    def column(row):
        spread = jnp.where(first == second, row.astype(F32), 0.0)
        return jnp.sum(spread, axis=1, keepdims=True).astype(jnp.int32)

    live = lane < column(counts)
    w = jnp.where(live, photons, 0.0)
    cell = jnp.where(live, cells, 0)
    column_of = cell // NG
    gz = cell - column_of * NG
    gx = column_of // 24
    gy = column_of - gx * 24
    place_in = ((gx >> 4) * 3 + (gy >> 3)) * 128 + (gx & 15) * 8 + (gy & 7)
    spot = (place_in * 512 + gz).astype(F32)
    same = (column(owned) == owned) & (first < second)
    rank = jnp.sum(jnp.where(same, 1.0, 0.0), axis=0, keepdims=True).astype(jnp.int32)
    place = owned * (2 * CAP) + rank
    rows = lax.broadcasted_iota(jnp.int32, (DEV, 32), 0)
    total = jnp.zeros((DEV, SLOTS), F32)
    for values, shift in ((w, 0), (spot, CAP)):
        hot = jnp.where(rows == place + shift, 1.0, 0.0).astype(BF16)
        hi = values.astype(BF16)
        rest = values - hi.astype(F32)
        mid = rest.astype(BF16)
        low = (rest - mid.astype(F32)).astype(BF16)
        total = total + ((mm(hot, hi, NN) + mm(hot, mid, NN)) + mm(hot, low, NN))
    return total.reshape(16, 2 * CAP, SLOTS)


KR = 16
STEP = KR * SLOTS


def one_hots(land, zp, col):
    spot = land[:, CAP:].reshape(16 * CAP, SLOTS).astype(jnp.int32)
    weight = land[:, :CAP].reshape(16 * CAP, SLOTS)
    hi = weight.astype(BF16).astype(F32)
    lo = weight - hi
    z = spot & 511
    col[...] = spot >> 9
    rows = lax.broadcasted_iota(jnp.int32, (NG, SLOTS), 0)
    for r in range(16 * CAP):
        hit = rows == z[r : r + 1, :]
        at = slice(r * SLOTS, (r + 1) * SLOTS)
        zp[:NG, at] = jnp.where(hit, hi[r : r + 1, :], 0.0).astype(BF16)
        zp[NG:, at] = jnp.where(hit, lo[r : r + 1, :], 0.0).astype(BF16)


def paint_group(g, zp, col, spread, acc):
    rows = lax.broadcasted_iota(jnp.int32, (NG, SLOTS), 0) + g * NG
    for kk in range(16 * CAP // KR):
        for r in range(KR):
            hit = rows == col[kk * KR + r : kk * KR + r + 1, :]
            spread[:, r * SLOTS : (r + 1) * SLOTS] = jnp.where(hit, 1.0, 0.0).astype(BF16)
        both = mm(zp[:, kk * STEP : (kk + 1) * STEP], spread[...], NT)
        part = both[:NG] + both[NG:]
        if kk == 0:
            acc[...] = part
        else:
            acc[...] += part


ROOT = 0.8660254037844386


def three(a, b, c, inverse):
    tr, ti = b[0] + c[0], b[1] + c[1]
    dr, di = ROOT * (b[0] - c[0]), ROOT * (b[1] - c[1])
    er, ei = a[0] - 0.5 * tr, a[1] - 0.5 * ti
    one, two = (er + di, ei - dr), (er - di, ei + dr)
    return (a[0] + tr, a[1] + ti), *((two, one) if inverse else (one, two))


def nine(v, inverse):
    v = list(v)
    for x in range(3):
        v[3 * x : 3 * x + 3] = three(*v[3 * x : 3 * x + 3], inverse)
    for y in range(3):
        v[y], v[y + 3], v[y + 6] = three(v[y], v[y + 3], v[y + 6], inverse)
    return v


def turn(v, c, s):
    return v[0] * c - v[1] * s, v[0] * s + v[1] * c


RB = 16
BATCH = 14


def everyone(body):
    me = lax.axis_index("px") * 16 + lax.axis_index("py")

    def one(t):
        other = me ^ ((t * 101) & (DEV - 1))
        body(other, (other >> 4, other & 15))

    def step(i, carry):
        for u in range(BATCH):
            one(1 + i * BATCH + u)
        return carry

    lax.fori_loop(0, (DEV - 2) // BATCH, step, 0)
    one(DEV - 1)


def fill_window(k, which, win):
    lane = lax.broadcasted_iota(jnp.int32, (RB, 128), 1)
    sub = lax.broadcasted_iota(jnp.int32, (RB, 128), 0)
    scale = jnp.where((k == 0) | (k == NG // 2), 1.0, 2.0) / float(NG) ** 3
    fz = signed(k)

    def step(i, carry):
        m, r = i // (DEV // RB), i % (DEV // RB)
        s = sub + r * RB
        bx = m // 3
        kx = (s >> 4) + 8 * bx + 24 * (lane >> 3)
        ky = (s & 15) + 16 * (m - 3 * bx) + 48 * (lane & 7)
        value = top_hat(signed(kx), signed(ky), fz) * scale
        win[which, pl.ds(pl.multiple_of(i * RB, RB), RB), :] = value
        return carry

    lax.fori_loop(0, CELLS // RB, step, 0)


def whole_body(
    ph, cell, count, owned, dens_hbm, table_hbm, tw_hbm, back_hbm, mats_hbm, result,
    dens, table, send, land, zp, col, spread, acc, f3, xg, xf, gs, fs, out,
    ys, rb, win, tw, back, ga, fa, mats, stack, wide, tall, uh, ul, vh, vl, ss, rs, sg, rg, sf, rf, sy, ry, own, sl,
):
    px, py = lax.axis_index("px"), lax.axis_index("py")
    me = px * 16 + py
    loads = [
        pltpu.make_async_copy(a, b, sl.at[i])
        for i, (a, b) in enumerate(((dens_hbm, dens), (table_hbm, table), (tw_hbm, tw), (back_hbm, back), (mats_hbm, mats)))
    ]
    ah, al, bh, bl, ch, cl, dh, dl = (mats.at[i] for i in range(8))
    loads[0].start()
    barrier = pltpu.get_barrier_semaphore()
    everyone(lambda i, to: pl.semaphore_signal(barrier, inc=1, device_id=to, device_id_type=MESH))
    for c in loads[1:]:
        c.start()
    send[...] = pack(ph[...], cell[...], count[...], owned[...])
    halo_own = pltpu.make_async_copy(send.at[py], land.at[py], own.at[0])
    halo_own.start()
    loads[0].wait()
    for m in range(9):
        xh, lh = m // 3, m % 3
        rows = [dens[(16 * xh + xl) * 24 + 8 * lh : (16 * xh + xl) * 24 + 8 * lh + 8, :] for xl in range(16)]
        hi, lo = cut(jnp.concatenate(rows, axis=0))
        at = slice(m * 128, (m + 1) * 128)
        stack[at, :NG] = hi
        stack[at, NG : 2 * NG] = lo
        stack[at, 2 * NG :] = hi
    pl.semaphore_wait(barrier, DEV - 1)
    for t in range(1, 16):
        to = (py + t) & 15
        pltpu.make_async_remote_copy(
            src_ref=send.at[to],
            dst_ref=land.at[py],
            send_sem=ss,
            recv_sem=rs,
            device_id=(px, to),
            device_id_type=MESH,
        ).start()
    loads[1].wait()
    res = mm(table[...], stack[...], NT)
    for c in range(3):
        xg[:, 0, c * CELLS : (c + 1) * CELLS] = res[c * DEV : (c + 1) * DEV]
    density_own = pltpu.make_async_copy(xg.at[me], gs.at[me], own.at[1])
    density_own.start()
    everyone(
        lambda i, to: pltpu.make_async_remote_copy(
            src_ref=xg.at[i],
            dst_ref=gs.at[me],
            send_sem=sg,
            recv_sem=rg,
            device_id=to,
            device_id_type=MESH,
        ).start()
    )
    fill_window(me + 1, 0, win)
    halo_own.wait()
    part = land.at[pl.ds(0, 15)]
    pltpu.make_async_copy(part, part, rs).wait()
    one_hots(land, zp, col)

    def one_group(g, carry):
        paint_group(g, zp, col, spread, acc)
        hi, lo = cut(acc[...])
        f3[:NG, :] = hi
        f3[NG : 2 * NG, :] = lo
        f3[2 * NG :, :] = hi
        res = mm(table[...], f3[...], NN)
        for c, first in enumerate((2 * DEV, 0, DEV)):
            xf[g, :, 0, c * NG : (c + 1) * NG] = res[first : first + DEV]
        pltpu.make_async_copy(xf.at[g, me], fs.at[g, me], own.at[2 + g]).start()
        everyone(
            lambda i, to: pltpu.make_async_remote_copy(
                src_ref=xf.at[g, i],
                dst_ref=fs.at[g, me],
                send_sem=sf.at[g],
                recv_sem=rf.at[g],
                device_id=to,
                device_id_type=MESH,
            ).start()
        )
        return carry

    lax.fori_loop(0, 3, one_group, 0)
    density_own.wait()
    for c in loads[2:]:
        c.wait()
    part = gs.at[pl.ds(0, DEV - 1)]
    pltpu.make_async_copy(part, part, rg).wait()

    def one_plane(p, carry):
        @pl.when(p == 0)
        def _():
            for c in range(2):
                wide[c * DEV : (c + 1) * DEV, :] = gs[:, 0, c * CELLS : (c + 1) * CELLS]

        @pl.when(p == 1)
        def _():
            for g in range(3):
                pltpu.make_async_copy(xf.at[g, me], fs.at[g, me], own.at[2 + g]).wait()
                part = fs.at[g, pl.ds(0, DEV - 1)]
                pltpu.make_async_copy(part, part, rf.at[g]).wait()
            wide[:DEV, :] = gs[:, 0, 2 * CELLS :]
            for g in range(3):
                wide[DEV:, g * NG : (g + 1) * NG] = fs[g, :, 0, :NG]

        @pl.when(p == 2)
        def _():
            for c in range(2):
                for g in range(3):
                    wide[c * DEV : (c + 1) * DEV, g * NG : (g + 1) * NG] = fs[g, :, 0, (c + 1) * NG : (c + 2) * NG]

        hi, lo = cut(wide[...])
        wide[...] = mm3(ah[...], al[...], hi, lo)

        def forward(i, inner):
            r = pl.multiple_of(i * RB, RB)
            v = []
            for m in range(9):
                cols = slice(m * 128, (m + 1) * 128)
                t = pl.ds(m * 128 + r, RB)
                u = (wide[pl.ds(r, RB), cols], wide[pl.ds(DEV + r, RB), cols])
                v.append(turn(u, tw[0, t, :], tw[1, t, :]))
            for m, u in enumerate(nine(v, False)):
                t = pl.ds(m * 128 + r, RB)
                for c, part in enumerate(turn(u, tw[2, t, :], tw[3, t, :])):
                    hi, lo = cut(part)
                    uh[t, c * 128 : (c + 1) * 128] = hi
                    ul[t, c * 128 : (c + 1) * 128] = lo
            return inner

        lax.fori_loop(0, DEV // RB, forward, 0)
        mid = mm3(uh[...], ul[...], ch[...], cl[...])
        this = win[p & 1]
        for c in range(2):
            hi, lo = cut(mid[:, c * 128 : (c + 1) * 128] * this)
            uh[:, c * 128 : (c + 1) * 128] = hi
            ul[:, c * 128 : (c + 1) * 128] = lo
        tall[...] = mm3(uh[...], ul[...], dh[...], dl[...])

        def backward(i, inner):
            r = pl.multiple_of(i * RB, RB)
            v = []
            for m in range(9):
                t = pl.ds(m * 128 + r, RB)
                v.append(turn((tall[t, :128], tall[t, 128:]), tw[2, t, :], -tw[3, t, :]))
            for m, u in enumerate(nine(v, True)):
                t = pl.ds(m * 128 + r, RB)
                cols = slice(m * 128, (m + 1) * 128)
                for c, part in enumerate(turn(u, tw[0, t, :], -tw[1, t, :])):
                    hi, lo = cut(part)
                    vh[pl.ds(c * DEV + r, RB), cols] = hi
                    vl[pl.ds(c * DEV + r, RB), cols] = lo
            return inner

        lax.fori_loop(0, DEV // RB, backward, 0)
        back = mm3(bh[...], bl[...], vh[...], vl[...])
        for c in range(2):
            for g in range(3):
                at = (2 * g + c) * NG
                ys[p, :, 0, at : at + NG] = back[c * DEV : (c + 1) * DEV, g * NG : (g + 1) * NG]
        pltpu.make_async_copy(ys.at[p, me], rb.at[p, me], own.at[5 + p]).start()
        @pl.when(p < 2)
        def _():
            everyone(
                lambda i, to: pltpu.make_async_remote_copy(
                    src_ref=ys.at[p, i],
                    dst_ref=rb.at[p, me],
                    send_sem=sy.at[p],
                    recv_sem=ry.at[p],
                    device_id=to,
                    device_id_type=MESH,
                ).start()
            )

        @pl.when(p == 2)
        def _():
            for g in range(3):
                cols = pl.ds(2 * g * NG, 2 * NG)
                everyone(
                    lambda i, to: pltpu.make_async_remote_copy(
                        src_ref=ys.at[2, i, :, cols],
                        dst_ref=rb.at[2, me, :, cols],
                        send_sem=sy.at[2 + g],
                        recv_sem=ry.at[2 + g],
                        device_id=to,
                        device_id_type=MESH,
                    ).start()
                )

        @pl.when(p == 0)
        def _():
            second = jnp.where(me < 63, 129 + me, jnp.where(me < 126, 66 + me, (me - 126) * (NG // 2)))
            fill_window(second, 1, win)

        return carry

    lax.fori_loop(0, 3, one_plane, 0)
    for p in range(2):
        pltpu.make_async_copy(ys.at[p, me], rb.at[p, me], own.at[5 + p]).wait()
        part = rb.at[p, pl.ds(0, DEV - 1)]
        pltpu.make_async_copy(part, part, ry.at[p]).wait()
    for i, (p, c) in enumerate(((0, 0), (0, 1), (1, 0), (1, 1))):
        spot = (i % 2) * DEV
        for g in range(3):
            wide[spot : spot + DEV, g * NG : (g + 1) * NG] = rb[p, :, 0, (2 * g + c) * NG : (2 * g + c + 1) * NG]
        hi, lo = cut(wide[spot : spot + DEV, :])
        at = (i % 3) * DEV
        if i < 3:
            stack[at : at + DEV, :] = hi
            stack[NG + at : NG + at + DEV, :] = lo
            stack[2 * NG + at : 2 * NG + at + DEV, :] = hi
        if i == 2:
            ga[...] = mm(back[...], stack[...], NN)
        if i == 3:
            cols = slice(2 * DEV, 3 * DEV)
            fa[...] = (mm(back[:, cols], hi, NN) + mm(back[:, cols], lo, NN)) + mm(back[:, 2 * NG + 2 * DEV :], hi, NN)
    part = send.at[pl.ds(0, 15)]
    pltpu.make_async_copy(part, part, ss).wait()
    part = xg.at[pl.ds(0, DEV - 1)]
    pltpu.make_async_copy(part, part, sg).wait()
    for g in range(3):
        part = xf.at[g, pl.ds(0, DEV - 1)]
        pltpu.make_async_copy(part, part, sf.at[g]).wait()
    for p in range(2):
        part = ys.at[p, pl.ds(0, DEV - 1)]
        pltpu.make_async_copy(part, part, sy.at[p]).wait()
    pltpu.make_async_copy(ys.at[2, me], rb.at[2, me], own.at[7]).wait()
    left = jnp.concatenate([back[:, i * NG : i * NG + 2 * DEV] for i in range(3)], axis=1)
    stores = []
    for xh in range(3):
        cols = slice(xh * NG, (xh + 1) * NG)
        part = rb.at[2, pl.ds(0, DEV - 1), :, pl.ds(2 * xh * NG, 2 * NG)]
        pltpu.make_async_copy(part, part, ry.at[2 + xh]).wait()
        for c in range(2):
            at = c * DEV
            wide[at : at + DEV, cols] = rb[2, :, 0, (2 * xh + c) * NG : (2 * xh + c + 1) * NG]
            hi, lo = cut(wide[at : at + DEV, cols])
            stack[at : at + DEV, cols] = hi
            stack[2 * DEV + at : 2 * DEV + at + DEV, cols] = lo
            stack[4 * DEV + at : 4 * DEV + at + DEV, cols] = hi
        f = fa[:, cols] + mm(left, stack[: 6 * DEV, cols], NN)
        frac = jnp.clip(f / jnp.maximum(ga[:, cols], 0.5), 0.0, 1.0)
        for lh in range(3):
            turned = frac[:, lh * 128 : (lh + 1) * 128].T
            for xl in range(16):
                at = (16 * xh + xl) * 24 + 8 * lh
                out[at : at + 8, :] = turned[xl * 8 : xl * 8 + 8, :]
        c = pltpu.make_async_copy(out.at[pl.ds(xh * NG, NG)], result.at[pl.ds(xh * NG, NG)], sl.at[xh])
        c.start()
        stores.append(c)
    for g in range(3):
        part = ys.at[2, pl.ds(0, DEV - 1), :, pl.ds(2 * g * NG, 2 * NG)]
        pltpu.make_async_copy(part, part, sy.at[2 + g]).wait()
    for c in stores:
        c.wait()


def sds(*shape, dtype=F32):
    return jax.ShapeDtypeStruct(shape, dtype)


def whole(halos, density, ahead, tw, back, mats):
    dma = pltpu.SemaphoreType.DMA
    plane = (DEV, 1, PLANE)
    anywhere, here = pl.BlockSpec(memory_space=pl.ANY), pl.BlockSpec(memory_space=VMEM)
    return pl.pallas_call(
        whole_body,
        out_shape=sds(CELLS, NG),
        in_specs=[here] * 4 + [anywhere] * 5,
        out_specs=anywhere,
        scratch_shapes=[
            VMEM((CELLS, NG), F32),
            VMEM((NG, 3 * NG), BF16),
            VMEM((16, 2 * CAP, SLOTS), F32),
            VMEM((16, 2 * CAP, SLOTS), F32),
            VMEM((2 * NG, 16 * CAP * SLOTS), BF16),
            VMEM((16 * CAP, SLOTS), jnp.int32),
            VMEM((NG, STEP), BF16),
            VMEM((NG, NG), F32),
            VMEM((3 * NG, NG), BF16),
            VMEM((DEV, 1, HALF), F32),
            VMEM((3, DEV, 1, CELLS), F32),
            VMEM((DEV, 1, HALF), F32),
            VMEM((3, DEV, 1, CELLS), F32),
            VMEM((CELLS, NG), F32),
            VMEM((3, *plane), F32),
            VMEM((3, *plane), F32),
            VMEM((2, CELLS, 128), F32),
            VMEM((4, CELLS, 128), F32),
            VMEM((NG, 3 * NG), BF16),
            VMEM((NG, CELLS), F32),
            VMEM((NG, CELLS), F32),
            VMEM((8, 256, 256), BF16),
            VMEM((3 * NG, CELLS), BF16),
            VMEM((256, CELLS), F32),
            VMEM((CELLS, 256), F32),
            VMEM((CELLS, 256), BF16),
            VMEM((CELLS, 256), BF16),
            VMEM((256, CELLS), BF16),
            VMEM((256, CELLS), BF16),
            dma,
            dma,
            dma,
            dma,
            dma((3,)),
            dma((3,)),
            dma((5,)),
            dma((5,)),
            dma((8,)),
            dma((5,)),
        ],
        compiler_params=pltpu.CompilerParams(vmem_limit_bytes=63 << 20, collective_id=1, has_side_effects=True),
        cost_estimate=pl.CostEstimate(flops=36 << 30, bytes_accessed=8 << 20, transcendentals=0),
        name="whole",
    )(*halos, density, ahead, tw, back, mats)


def on_device(photons, halo_cells, halo_counts, owners, density):
    table = z_table()
    ahead, back = stacked(table, 1), stacked(table.T, 1)
    mats = []
    for m in (row_matrix(1), row_matrix(-1), lane_matrix(1), lane_matrix(-1)):
        mats += cut_np(m)
    mats = jnp.asarray(np.stack(mats))

    halos = (photons, halo_cells, halo_counts.reshape(1, 32), owners.reshape(1, 32))
    out = whole(halos, density.reshape(CELLS, NG), ahead, jnp.asarray(twiddles()), back, mats)
    return out.reshape(48, 24, NG)


def solution(mesh):
    placed = (
        P(("px", "py"), None),
        P(("px", "py"), None),
        P(("px", "py")),
        P(("px", "py"), None),
        P("px", "py", None),
    )
    return jax.shard_map(
        on_device, mesh=mesh, in_specs=placed, out_specs=P("px", "py", None), check_vma=False
    )
```

```python
import functools

import jax
import jax.numpy as jnp
import numpy as np
from jax import lax
from jax.experimental import pallas as pl
from jax.experimental.pallas import tpu as pltpu
from jax.sharding import PartitionSpec as P

NG = 384
SLOTS = 128
CAP = 4
RADIUS = 20
DEV = 128
CELLS = 1152
PLANE = 2 * CELLS
HALF = 3 * CELLS
LIMIT = 60 * 1024 * 1024
F32 = jnp.float32
BF16 = jnp.bfloat16
VMEM = pltpu.VMEM
MESH = pl.DeviceIdType.MESH


def cut(v):
    hi = v.astype(BF16)
    return hi, (v - hi.astype(F32)).astype(BF16)


def cut_np(v):
    v = np.asarray(v, np.float32)
    hi = v.astype(jnp.bfloat16)
    lo = (v - hi.astype(np.float32)).astype(jnp.bfloat16)
    return hi, lo


NN = (((1,), (0,)), ((), ()))
NT = (((1,), (1,)), ((), ()))


def mm(a, b, dims):
    return lax.dot_general(a, b, dims, preferred_element_type=F32)


def mm3(ah, al, bh, bl, dims=NN):
    return mm(ah, bh, dims) + (mm(ah, bl, dims) + mm(al, bh, dims))


def z_table():
    k = np.arange(1, NG // 2)[:, None] * np.arange(NG)[None]
    angle = 2 * np.pi * (k % NG) / NG
    c, s = np.cos(angle), np.sin(angle)
    ends = np.stack([np.ones(NG), 1.0 - 2.0 * (np.arange(NG) % 2)])
    return np.concatenate([c[:DEV], s[:DEV], c[DEV:], s[DEV:], ends])


def stacked(v, axis):
    hi, lo = cut_np(v)
    return jnp.asarray(np.concatenate([hi, hi, lo], axis=axis))


def mix(left, right):
    i = np.arange(left * right)
    a, b = i // right, i % right
    ph = -2j * np.pi * (np.outer(a, a) / left + np.outer(b, b) / right)
    return np.exp(ph)


def row_matrix(sign):
    m = mix(8, 16)
    re, im = m.real, sign * m.imag
    return np.block([[re, -im], [im, re]])


def lane_matrix(sign):
    m = mix(16, 8)
    re, im = m.real, sign * m.imag
    return np.block([[re, im], [-im, re]])


def twiddles():
    row, lane = np.arange(CELLS)[:, None], np.arange(128)[None]
    m, s = row // 128, row % 128
    ax, ay, bx, by, cx, cy = s // 16, s % 16, m // 3, m % 3, lane // 8, lane % 8
    one = (ax * bx * 16 + ay * by * 8 + 0 * lane) * (2 * np.pi / NG)
    two = (cx * (ax + 8 * bx) + cy * (ay + 16 * by)) * (2 * np.pi / NG)
    return np.stack([np.cos(one), -np.sin(one), np.cos(two), -np.sin(two)]).astype(np.float32)


def signed(k):
    return jnp.where(k < NG // 2, k, k - NG).astype(F32)


def top_hat(freq_x, freq_y, freq_z):
    radial = jnp.sqrt(freq_x * freq_x + freq_y * freq_y + freq_z * freq_z) * (2.0 * jnp.pi * RADIUS / NG)
    safe = jnp.where(radial > 0, radial, 1.0)
    value = 3.0 * (jnp.sin(safe) - safe * jnp.cos(safe)) / (safe * safe * safe)
    return jnp.where(radial > 0, value, 1.0)


def pack(photons, cells, counts, owned):
    lane = lax.broadcasted_iota(jnp.int32, (32, SLOTS), 1)
    first = lax.broadcasted_iota(jnp.int32, (32, 32), 0)
    second = lax.broadcasted_iota(jnp.int32, (32, 32), 1)

    def column(row):
        spread = jnp.where(first == second, row.astype(F32), 0.0)
        return jnp.sum(spread, axis=1, keepdims=True).astype(jnp.int32)

    live = lane < column(counts)
    w = jnp.where(live, photons, 0.0)
    cell = jnp.where(live, cells, 0)
    column_of = cell // NG
    gz = cell - column_of * NG
    gx = column_of // 24
    gy = column_of - gx * 24
    place_in = ((gx >> 4) * 3 + (gy >> 3)) * 128 + (gx & 15) * 8 + (gy & 7)
    spot = (place_in * 512 + gz).astype(F32)
    same = (column(owned) == owned) & (first < second)
    rank = jnp.sum(jnp.where(same, 1.0, 0.0), axis=0, keepdims=True).astype(jnp.int32)
    place = owned * (2 * CAP) + rank
    rows = lax.broadcasted_iota(jnp.int32, (DEV, 32), 0)
    total = jnp.zeros((DEV, SLOTS), F32)
    for values, shift in ((w, 0), (spot, CAP)):
        hot = jnp.where(rows == place + shift, 1.0, 0.0).astype(BF16)
        hi = values.astype(BF16)
        rest = values - hi.astype(F32)
        mid = rest.astype(BF16)
        low = (rest - mid.astype(F32)).astype(BF16)
        total = total + ((mm(hot, hi, NN) + mm(hot, mid, NN)) + mm(hot, low, NN))
    return total.reshape(16, 2 * CAP, SLOTS)


KR = 16
STEP = KR * SLOTS


def one_hots(land, zp, col):
    spot = land[:, CAP:].reshape(16 * CAP, SLOTS).astype(jnp.int32)
    weight = land[:, :CAP].reshape(16 * CAP, SLOTS)
    hi = weight.astype(BF16).astype(F32)
    lo = weight - hi
    z = spot & 511
    col[...] = spot >> 9
    rows = lax.broadcasted_iota(jnp.int32, (NG, SLOTS), 0)
    for r in range(16 * CAP):
        hit = rows == z[r : r + 1, :]
        at = slice(r * SLOTS, (r + 1) * SLOTS)
        zp[:NG, at] = jnp.where(hit, hi[r : r + 1, :], 0.0).astype(BF16)
        zp[NG:, at] = jnp.where(hit, lo[r : r + 1, :], 0.0).astype(BF16)


def paint_group(g, zp, col, spread, acc):
    rows = lax.broadcasted_iota(jnp.int32, (NG, SLOTS), 0) + g * NG
    for kk in range(16 * CAP // KR):
        for r in range(KR):
            hit = rows == col[kk * KR + r : kk * KR + r + 1, :]
            spread[:, r * SLOTS : (r + 1) * SLOTS] = jnp.where(hit, 1.0, 0.0).astype(BF16)
        both = mm(zp[:, kk * STEP : (kk + 1) * STEP], spread[...], NT)
        part = both[:NG] + both[NG:]
        if kk == 0:
            acc[...] = part
        else:
            acc[...] += part


ROOT = 0.8660254037844386


def three(a, b, c, inverse):
    tr, ti = b[0] + c[0], b[1] + c[1]
    dr, di = ROOT * (b[0] - c[0]), ROOT * (b[1] - c[1])
    er, ei = a[0] - 0.5 * tr, a[1] - 0.5 * ti
    one, two = (er + di, ei - dr), (er - di, ei + dr)
    return (a[0] + tr, a[1] + ti), *((two, one) if inverse else (one, two))


def nine(v, inverse):
    v = list(v)
    for x in range(3):
        v[3 * x : 3 * x + 3] = three(*v[3 * x : 3 * x + 3], inverse)
    for y in range(3):
        v[y], v[y + 3], v[y + 6] = three(v[y], v[y + 3], v[y + 6], inverse)
    return v


def turn(v, c, s):
    return v[0] * c - v[1] * s, v[0] * s + v[1] * c


RB = 16
BATCH = 14


def everyone(body):
    me = lax.axis_index("px") * 16 + lax.axis_index("py")

    def one(t):
        other = me ^ ((t * 101) & (DEV - 1))
        body(other, (other >> 4, other & 15))

    def step(i, carry):
        for u in range(BATCH):
            one(1 + i * BATCH + u)
        return carry

    lax.fori_loop(0, (DEV - 2) // BATCH, step, 0)
    one(DEV - 1)


def fill_window(k, which, win):
    lane = lax.broadcasted_iota(jnp.int32, (RB, 128), 1)
    sub = lax.broadcasted_iota(jnp.int32, (RB, 128), 0)
    scale = jnp.where((k == 0) | (k == NG // 2), 1.0, 2.0) / float(NG) ** 3
    fz = signed(k)

    def step(i, carry):
        m, r = i // (DEV // RB), i % (DEV // RB)
        s = sub + r * RB
        bx = m // 3
        kx = (s >> 4) + 8 * bx + 24 * (lane >> 3)
        ky = (s & 15) + 16 * (m - 3 * bx) + 48 * (lane & 7)
        value = top_hat(signed(kx), signed(ky), fz) * scale
        win[which, pl.ds(pl.multiple_of(i * RB, RB), RB), :] = value
        return carry

    lax.fori_loop(0, CELLS // RB, step, 0)


def whole_body(
    ph, cell, count, owned, dens_hbm, table_hbm, tw_hbm, back_hbm, mats_hbm, result,
    dens, table, send, land, zp, col, spread, acc, f3, xg, xf, gs, fs, out,
    ys, rb, win, tw, back, ga, fa, mats, stack, wide, tall, uh, ul, vh, vl, ss, rs, sg, rg, sf, rf, sy, ry, own, sl,
):
    px, py = lax.axis_index("px"), lax.axis_index("py")
    me = px * 16 + py
    loads = [
        pltpu.make_async_copy(a, b, sl.at[i])
        for i, (a, b) in enumerate(((dens_hbm, dens), (table_hbm, table), (tw_hbm, tw), (back_hbm, back), (mats_hbm, mats)))
    ]
    ah, al, bh, bl, ch, cl, dh, dl = (mats.at[i] for i in range(8))
    loads[0].start()
    barrier = pltpu.get_barrier_semaphore()
    everyone(lambda i, to: pl.semaphore_signal(barrier, inc=1, device_id=to, device_id_type=MESH))
    for c in loads[1:]:
        c.start()
    send[...] = pack(ph[...], cell[...], count[...], owned[...])
    halo_own = pltpu.make_async_copy(send.at[py], land.at[py], own.at[0])
    halo_own.start()
    loads[0].wait()
    for m in range(9):
        xh, lh = m // 3, m % 3
        rows = [dens[(16 * xh + xl) * 24 + 8 * lh : (16 * xh + xl) * 24 + 8 * lh + 8, :] for xl in range(16)]
        hi, lo = cut(jnp.concatenate(rows, axis=0))
        at = slice(m * 128, (m + 1) * 128)
        stack[at, :NG] = hi
        stack[at, NG : 2 * NG] = lo
        stack[at, 2 * NG :] = hi
    pl.semaphore_wait(barrier, DEV - 1)
    for t in range(1, 16):
        to = (py + t) & 15
        pltpu.make_async_remote_copy(
            src_ref=send.at[to],
            dst_ref=land.at[py],
            send_sem=ss,
            recv_sem=rs,
            device_id=(px, to),
            device_id_type=MESH,
        ).start()
    loads[1].wait()
    res = mm(table[...], stack[...], NT)
    for c in range(3):
        xg[:, 0, c * CELLS : (c + 1) * CELLS] = res[c * DEV : (c + 1) * DEV]
    density_own = pltpu.make_async_copy(xg.at[me], gs.at[me], own.at[1])
    density_own.start()
    everyone(
        lambda i, to: pltpu.make_async_remote_copy(
            src_ref=xg.at[i],
            dst_ref=gs.at[me],
            send_sem=sg,
            recv_sem=rg,
            device_id=to,
            device_id_type=MESH,
        ).start()
    )
    halo_own.wait()
    part = land.at[pl.ds(0, 15)]
    pltpu.make_async_copy(part, part, rs).wait()
    one_hots(land, zp, col)

    def one_group(g, carry):
        paint_group(g, zp, col, spread, acc)
        hi, lo = cut(acc[...])
        f3[:NG, :] = hi
        f3[NG : 2 * NG, :] = lo
        f3[2 * NG :, :] = hi
        res = mm(table[...], f3[...], NN)
        for c, first in enumerate((2 * DEV, 0, DEV)):
            xf[g, :, 0, c * NG : (c + 1) * NG] = res[first : first + DEV]
        pltpu.make_async_copy(xf.at[g, me], fs.at[g, me], own.at[2 + g]).start()
        everyone(
            lambda i, to: pltpu.make_async_remote_copy(
                src_ref=xf.at[g, i],
                dst_ref=fs.at[g, me],
                send_sem=sf.at[g],
                recv_sem=rf.at[g],
                device_id=to,
                device_id_type=MESH,
            ).start()
        )
        return carry

    lax.fori_loop(0, 3, one_group, 0)
    fill_window(me + 1, 0, win)
    density_own.wait()
    for c in loads[2:]:
        c.wait()
    part = gs.at[pl.ds(0, DEV - 1)]
    pltpu.make_async_copy(part, part, rg).wait()

    def one_plane(p, carry):
        @pl.when(p == 0)
        def _():
            for c in range(2):
                wide[c * DEV : (c + 1) * DEV, :] = gs[:, 0, c * CELLS : (c + 1) * CELLS]

        @pl.when(p == 1)
        def _():
            for g in range(3):
                pltpu.make_async_copy(xf.at[g, me], fs.at[g, me], own.at[2 + g]).wait()
                part = fs.at[g, pl.ds(0, DEV - 1)]
                pltpu.make_async_copy(part, part, rf.at[g]).wait()
            wide[:DEV, :] = gs[:, 0, 2 * CELLS :]
            for g in range(3):
                wide[DEV:, g * NG : (g + 1) * NG] = fs[g, :, 0, :NG]

        @pl.when(p == 2)
        def _():
            for c in range(2):
                for g in range(3):
                    wide[c * DEV : (c + 1) * DEV, g * NG : (g + 1) * NG] = fs[g, :, 0, (c + 1) * NG : (c + 2) * NG]

        hi, lo = cut(wide[...])
        wide[...] = mm3(ah[...], al[...], hi, lo)

        def forward(i, inner):
            r = pl.multiple_of(i * RB, RB)
            v = []
            for m in range(9):
                cols = slice(m * 128, (m + 1) * 128)
                t = pl.ds(m * 128 + r, RB)
                u = (wide[pl.ds(r, RB), cols], wide[pl.ds(DEV + r, RB), cols])
                v.append(turn(u, tw[0, t, :], tw[1, t, :]))
            for m, u in enumerate(nine(v, False)):
                t = pl.ds(m * 128 + r, RB)
                for c, part in enumerate(turn(u, tw[2, t, :], tw[3, t, :])):
                    hi, lo = cut(part)
                    uh[t, c * 128 : (c + 1) * 128] = hi
                    ul[t, c * 128 : (c + 1) * 128] = lo
            return inner

        lax.fori_loop(0, DEV // RB, forward, 0)
        mid = mm3(uh[...], ul[...], ch[...], cl[...])
        this = win[p & 1]
        for c in range(2):
            hi, lo = cut(mid[:, c * 128 : (c + 1) * 128] * this)
            uh[:, c * 128 : (c + 1) * 128] = hi
            ul[:, c * 128 : (c + 1) * 128] = lo
        tall[...] = mm3(uh[...], ul[...], dh[...], dl[...])

        def backward(i, inner):
            r = pl.multiple_of(i * RB, RB)
            v = []
            for m in range(9):
                t = pl.ds(m * 128 + r, RB)
                v.append(turn((tall[t, :128], tall[t, 128:]), tw[2, t, :], -tw[3, t, :]))
            for m, u in enumerate(nine(v, True)):
                t = pl.ds(m * 128 + r, RB)
                cols = slice(m * 128, (m + 1) * 128)
                for c, part in enumerate(turn(u, tw[0, t, :], -tw[1, t, :])):
                    hi, lo = cut(part)
                    vh[pl.ds(c * DEV + r, RB), cols] = hi
                    vl[pl.ds(c * DEV + r, RB), cols] = lo
            return inner

        lax.fori_loop(0, DEV // RB, backward, 0)
        back = mm3(bh[...], bl[...], vh[...], vl[...])
        for c in range(2):
            for g in range(3):
                at = (2 * g + c) * NG
                ys[p, :, 0, at : at + NG] = back[c * DEV : (c + 1) * DEV, g * NG : (g + 1) * NG]
        pltpu.make_async_copy(ys.at[p, me], rb.at[p, me], own.at[5 + p]).start()
        @pl.when(p < 2)
        def _():
            everyone(
                lambda i, to: pltpu.make_async_remote_copy(
                    src_ref=ys.at[p, i],
                    dst_ref=rb.at[p, me],
                    send_sem=sy.at[p],
                    recv_sem=ry.at[p],
                    device_id=to,
                    device_id_type=MESH,
                ).start()
            )

        @pl.when(p == 2)
        def _():
            for g in range(3):
                cols = pl.ds(2 * g * NG, 2 * NG)
                everyone(
                    lambda i, to: pltpu.make_async_remote_copy(
                        src_ref=ys.at[2, i, :, cols],
                        dst_ref=rb.at[2, me, :, cols],
                        send_sem=sy.at[2 + g],
                        recv_sem=ry.at[2 + g],
                        device_id=to,
                        device_id_type=MESH,
                    ).start()
                )

        @pl.when(p == 0)
        def _():
            second = jnp.where(me < 63, 129 + me, jnp.where(me < 126, 66 + me, (me - 126) * (NG // 2)))
            fill_window(second, 1, win)

        return carry

    lax.fori_loop(0, 3, one_plane, 0)
    for p in range(2):
        pltpu.make_async_copy(ys.at[p, me], rb.at[p, me], own.at[5 + p]).wait()
        part = rb.at[p, pl.ds(0, DEV - 1)]
        pltpu.make_async_copy(part, part, ry.at[p]).wait()
    for i, (p, c) in enumerate(((0, 0), (0, 1), (1, 0), (1, 1))):
        spot = (i % 2) * DEV
        for g in range(3):
            wide[spot : spot + DEV, g * NG : (g + 1) * NG] = rb[p, :, 0, (2 * g + c) * NG : (2 * g + c + 1) * NG]
        hi, lo = cut(wide[spot : spot + DEV, :])
        at = (i % 3) * DEV
        if i < 3:
            stack[at : at + DEV, :] = hi
            stack[NG + at : NG + at + DEV, :] = lo
            stack[2 * NG + at : 2 * NG + at + DEV, :] = hi
        if i == 2:
            ga[...] = mm(back[...], stack[...], NN)
        if i == 3:
            cols = slice(2 * DEV, 3 * DEV)
            fa[...] = (mm(back[:, cols], hi, NN) + mm(back[:, cols], lo, NN)) + mm(back[:, 2 * NG + 2 * DEV :], hi, NN)
    part = send.at[pl.ds(0, 15)]
    pltpu.make_async_copy(part, part, ss).wait()
    part = xg.at[pl.ds(0, DEV - 1)]
    pltpu.make_async_copy(part, part, sg).wait()
    for g in range(3):
        part = xf.at[g, pl.ds(0, DEV - 1)]
        pltpu.make_async_copy(part, part, sf.at[g]).wait()
    for p in range(2):
        part = ys.at[p, pl.ds(0, DEV - 1)]
        pltpu.make_async_copy(part, part, sy.at[p]).wait()
    pltpu.make_async_copy(ys.at[2, me], rb.at[2, me], own.at[7]).wait()
    left = jnp.concatenate([back[:, i * NG : i * NG + 2 * DEV] for i in range(3)], axis=1)
    stores = []
    for xh in range(3):
        cols = slice(xh * NG, (xh + 1) * NG)
        part = rb.at[2, pl.ds(0, DEV - 1), :, pl.ds(2 * xh * NG, 2 * NG)]
        pltpu.make_async_copy(part, part, ry.at[2 + xh]).wait()
        for c in range(2):
            at = c * DEV
            wide[at : at + DEV, cols] = rb[2, :, 0, (2 * xh + c) * NG : (2 * xh + c + 1) * NG]
            hi, lo = cut(wide[at : at + DEV, cols])
            stack[at : at + DEV, cols] = hi
            stack[2 * DEV + at : 2 * DEV + at + DEV, cols] = lo
            stack[4 * DEV + at : 4 * DEV + at + DEV, cols] = hi
        f = fa[:, cols] + mm(left, stack[: 6 * DEV, cols], NN)
        frac = jnp.clip(f / jnp.maximum(ga[:, cols], 0.5), 0.0, 1.0)
        for lh in range(3):
            turned = frac[:, lh * 128 : (lh + 1) * 128].T
            for xl in range(16):
                at = (16 * xh + xl) * 24 + 8 * lh
                out[at : at + 8, :] = turned[xl * 8 : xl * 8 + 8, :]
        c = pltpu.make_async_copy(out.at[pl.ds(xh * NG, NG)], result.at[pl.ds(xh * NG, NG)], sl.at[xh])
        c.start()
        stores.append(c)
    for g in range(3):
        part = ys.at[2, pl.ds(0, DEV - 1), :, pl.ds(2 * g * NG, 2 * NG)]
        pltpu.make_async_copy(part, part, sy.at[2 + g]).wait()
    for c in stores:
        c.wait()


def sds(*shape, dtype=F32):
    return jax.ShapeDtypeStruct(shape, dtype)


def whole(halos, density, ahead, tw, back, mats):
    dma = pltpu.SemaphoreType.DMA
    plane = (DEV, 1, PLANE)
    anywhere, here = pl.BlockSpec(memory_space=pl.ANY), pl.BlockSpec(memory_space=VMEM)
    return pl.pallas_call(
        whole_body,
        out_shape=sds(CELLS, NG),
        in_specs=[here] * 4 + [anywhere] * 5,
        out_specs=anywhere,
        scratch_shapes=[
            VMEM((CELLS, NG), F32),
            VMEM((NG, 3 * NG), BF16),
            VMEM((16, 2 * CAP, SLOTS), F32),
            VMEM((16, 2 * CAP, SLOTS), F32),
            VMEM((2 * NG, 16 * CAP * SLOTS), BF16),
            VMEM((16 * CAP, SLOTS), jnp.int32),
            VMEM((NG, STEP), BF16),
            VMEM((NG, NG), F32),
            VMEM((3 * NG, NG), BF16),
            VMEM((DEV, 1, HALF), F32),
            VMEM((3, DEV, 1, CELLS), F32),
            VMEM((DEV, 1, HALF), F32),
            VMEM((3, DEV, 1, CELLS), F32),
            VMEM((CELLS, NG), F32),
            VMEM((3, *plane), F32),
            VMEM((3, *plane), F32),
            VMEM((2, CELLS, 128), F32),
            VMEM((4, CELLS, 128), F32),
            VMEM((NG, 3 * NG), BF16),
            VMEM((NG, CELLS), F32),
            VMEM((NG, CELLS), F32),
            VMEM((8, 256, 256), BF16),
            VMEM((3 * NG, CELLS), BF16),
            VMEM((256, CELLS), F32),
            VMEM((CELLS, 256), F32),
            VMEM((CELLS, 256), BF16),
            VMEM((CELLS, 256), BF16),
            VMEM((256, CELLS), BF16),
            VMEM((256, CELLS), BF16),
            dma,
            dma,
            dma,
            dma,
            dma((3,)),
            dma((3,)),
            dma((5,)),
            dma((5,)),
            dma((8,)),
            dma((5,)),
        ],
        compiler_params=pltpu.CompilerParams(vmem_limit_bytes=63 << 20, collective_id=1, has_side_effects=True),
        cost_estimate=pl.CostEstimate(flops=36 << 30, bytes_accessed=8 << 20, transcendentals=0),
        name="whole",
    )(*halos, density, ahead, tw, back, mats)


def on_device(photons, halo_cells, halo_counts, owners, density):
    table = z_table()
    ahead, back = stacked(table, 1), stacked(table.T, 1)
    mats = []
    for m in (row_matrix(1), row_matrix(-1), lane_matrix(1), lane_matrix(-1)):
        mats += cut_np(m)
    mats = jnp.asarray(np.stack(mats))

    halos = (photons, halo_cells, halo_counts.reshape(1, 32), owners.reshape(1, 32))
    out = whole(halos, density.reshape(CELLS, NG), ahead, jnp.asarray(twiddles()), back, mats)
    return out.reshape(48, 24, NG)


def solution(mesh):
    placed = (
        P(("px", "py"), None),
        P(("px", "py"), None),
        P(("px", "py")),
        P(("px", "py"), None),
        P("px", "py", None),
    )
    return jax.shard_map(
        on_device, mesh=mesh, in_specs=placed, out_specs=P("px", "py", None), check_vma=False
    )
```
